32 devices in a mesh: row: 2 (over x), col: 16 (over z, y, core).
Axes of the slice: x: 2, y: 2, z: 4, core: 2. Of those that a mesh axis runs over, the one named last changes fastest.
Arguments:
- eigvecs: float32 [16384, 4096], P('row', 'col'), may hold values from -6 to 6
- v_panels: float32 [8, 16384, 256], P(None, 'row', 'col'), as said below
- t_panels: float32 [8, 256, 256], P(None, None, 'col'), as said below
Outputs:
- rotated: float32 [16384, 4096], P('row', 'col')
The draws below stay inside these ranges and needn't reach their ends.
Inputs may be any that keep to these rules, and one draw needn't show every extreme that they name: `v_panels`: in panel k, vector j is zero in rows above k * 256 + j + 1, equals 1 in that row and is dense below it. t_panels[k] is upper triangular and V_k t_panels[k] V_k^T = I minus the product of the panel's 256 Householder reflections, each I - 2 v v^T / (v^T v), taken in the order of j; its diagonal lies in (0, 2].
All inputs are finite; a program needn't handle non-finite values.
Results may differ from the reference program's by a relative error of at most 0.00015.
Values sent between devices are 32-bit elements; how exact they have to be, the bound alone decides.
A program may use at most 192 MiB of HBM per device.

```python
import math
import jax
import jax.numpy as jnp
from jax import lax

ORDER = 16384
PANEL_W = 256
PANELS = 8
COLS = 4096


def householder_panels(key):
    noise = jax.random.normal(jax.random.fold_in(key, 7), (PANELS, ORDER, PANEL_W), jnp.float32) / math.sqrt(ORDER)
    rows_at = lax.broadcasted_iota(jnp.int32, (PANELS, ORDER, PANEL_W), 1)
    column_at = lax.broadcasted_iota(jnp.int32, (PANELS, ORDER, PANEL_W), 2)
    panel_at = lax.broadcasted_iota(jnp.int32, (PANELS, ORDER, PANEL_W), 0)
    unit_row = panel_at * PANEL_W + column_at + 1
    return jnp.where(rows_at > unit_row, noise, jnp.where(rows_at == unit_row, 1.0, 0.0)).astype(jnp.float32)


def draw_v_panels(key, part):
    return householder_panels(key)


def draw_t_panels(key, part):
    vectors = householder_panels(key)
    gram = jnp.einsum('knb,knc->kbc', vectors, vectors, precision=lax.Precision.HIGHEST)
    identity = jnp.eye(PANEL_W, dtype=jnp.float32)
    inverse_factor = jnp.triu(gram, 1) + 0.5 * gram * identity
    eye_stack = jnp.broadcast_to(identity, (PANELS, PANEL_W, PANEL_W))
    factor = lax.linalg.triangular_solve(inverse_factor, eye_stack, left_side=True, lower=False)
    return jnp.triu(factor).astype(jnp.float32)


def block_scale(own_key, shape, split, least, largest):
    level = 1.0
    for position, shards_of in split:
        draws = jax.random.uniform(jax.random.fold_in(jax.random.fold_in(own_key, 6), position), (shards_of,), jnp.float32, least / len(split), largest / len(split))
        level = level * jnp.repeat(jnp.exp(draws), shape[position] // shards_of).reshape((-1,) + (1,) * (len(shape) - 1 - position))
    return level


def scatter_about(rng, shape, deviation, most, pieces=(), held_as=jnp.bfloat16):
    loudness = block_scale(rng, shape, pieces, -0.22, 0.18) if pieces else 1.0
    drawn = jax.random.normal(rng, shape, jnp.float32) * deviation * loudness
    return jnp.minimum(jnp.maximum(drawn, -most), most).astype(held_as)


def setup_inputs(seed: int = 0) -> dict:
    keys = jax.random.split(jax.random.key(seed), 4)
    return {
        "eigvecs": scatter_about(keys[0], (ORDER, COLS), 1.0, 6.0, ((0, 2), (1, 16)), jnp.float32),
        "v_panels": draw_v_panels(jax.random.fold_in(keys[3], 71), 0),
        "t_panels": draw_t_panels(jax.random.fold_in(keys[3], 71), 0),
    }


def reference(eigvecs, v_panels, t_panels):
    current = eigvecs
    for panel_index in reversed(range(PANELS)):
        vectors = v_panels[panel_index]
        projected = jnp.dot(vectors.T.astype(jnp.float32), current.astype(jnp.float32), preferred_element_type=jnp.float32, precision=lax.Precision.HIGHEST)
        scaled = jnp.dot(t_panels[panel_index].astype(jnp.float32), projected.astype(jnp.float32), preferred_element_type=jnp.float32, precision=lax.Precision.HIGHEST)
        current = current - jnp.dot(vectors.astype(jnp.float32), scaled.astype(jnp.float32), preferred_element_type=jnp.float32, precision=lax.Precision.HIGHEST)
    return current
```

```python
import functools

import jax
import jax.numpy as jnp
from jax import lax
from jax.experimental import pallas as pl
from jax.experimental.pallas import tpu as pltpu
from jax.sharding import PartitionSpec as P

SLOTS = 8
AHEAD = 2
MESH = pl.DeviceIdType.MESH


def halves(x):
    high = x.astype(jnp.bfloat16)
    return high, (x - high.astype(jnp.float32)).astype(jnp.bfloat16)


def dot3(left, right, left_axis, right_axis):
    def one(a, b):
        return lax.dot_general(
            a, b, (((left_axis,), (right_axis,)), ((), ())), preferred_element_type=jnp.float32
        )

    (lh, ll), (rh, rl) = left, right
    return one(lh, rh) + (one(ll, rh) + one(lh, rl))


def kernel(shape, z_hbm, v_ref, t_ref, out_ref, g_ref, gt_ref, zbuf, vbuf, tbuf, acc, psend, precv, *sems):
    groups, A, B = shape
    recv, su, sd, sy, sc, lsem, zsem, psnd, prcv, town, tsnd, trcv, tlsem = sems
    panels, H, sub, rows = v_ref.shape
    members = 2 * A * B
    width = H * members * sub
    units = panels * H
    share = panels // groups
    tiles = rows // 128
    spare = (B - 1) * A - (A - 1)
    whole = 2 * max((A - 1) * (B - 1), 1)
    side = min(max((tiles * spare + whole // 2) // whole, 1), tiles - 1)
    cut = (tiles - side) * 128
    lanes = (pl.ds(0, cut), pl.ds(cut, rows - cut))
    tile = min(rows, 1024)
    me = lax.axis_index("col")
    my_row = lax.axis_index("row")
    c = lax.rem(me, 2)
    b = lax.rem(me // 2, B)
    a = me // (2 * B)
    mine = pl.ds(my_row * share, share)

    def index(aa, bb, cc):
        return (aa * B + bb) * 2 + cc

    def place(u, owner, q):
        if q == 2:
            return gt_ref.at[mine, :, owner]
        return g_ref.at[panels - 1 - u // H, lax.rem(u, H), owner, :, lanes[q]]

    def first(u, q):
        if q == 2:
            return t_ref.at[mine]
        return v_ref.at[panels - 1 - u // H, lax.rem(u, H), :, lanes[q]]

    def landed(u, owner, q):
        sl = lax.rem(u, SLOTS)
        spot = place(u, owner, q)
        pltpu.make_async_remote_copy(
            src_ref=spot,
            dst_ref=spot,
            send_sem=sc.at[sl, q, 0],
            recv_sem=recv.at[sl, q, owner],
            device_id={"col": index(a, b, 1 - c)},
            device_id_type=MESH,
        ).wait_recv()

    def hop(u, h, go):
        sl = lax.rem(u, SLOTS)

        def move(owner, q, own, target, sem):
            copy = pltpu.make_async_remote_copy(
                src_ref=first(u, q) if own else place(u, owner, q),
                dst_ref=place(u, owner, q),
                send_sem=sem,
                recv_sem=recv.at[sl, q, owner],
                device_id={"col": target},
                device_id_type=MESH,
            )
            if go:
                copy.start()
            else:
                copy.wait_send()

        def arrive(owner, q):
            if go:
                landed(u, owner, q)

        def along(sg, owner, q, own, cid):
            if sg >= 0:

                @pl.when(a < A - 1)
                def _():
                    move(owner, q, own, index(a + 1, b, c), su.at[sl, q, cid])

            if sg <= 0:

                @pl.when(a > 0)
                def _():
                    move(owner, q, own, index(a - 1, b, c), sd.at[sl, q, cid])

        def across(owner, q, own, slot):
            for j in range(1, B):
                move(owner, q, own, index(a, lax.rem(b + j, B), c), sy.at[sl, slot, j - 1])

        def over(owner, q, own, cid):
            move(owner, q, own, index(a, b, 1 - c), sc.at[sl, q, cid])

        def factors(body):
            pl.when(u == 0)(body)

        def signs(d):
            return (1, -1) if d else (0,)

        if h == 0:
            cid = a * B + b
            across(me, 1, True, A)
            along(0, me, 0, True, cid)
            along(0, me, 1, True, cid)
            across(me, 0, True, a)
            over(me, 0, True, cid)
            over(me, 1, True, cid)

            @factors
            def _():
                along(0, me, 2, True, cid)
                across(me, 2, True, A + 1 + a)
                over(me, 2, True, cid)

            return

        def facing(d, body):
            if d < A:
                for sg in signs(d):
                    at = a - sg * d
                    if d == 0:
                        body(sg, at)
                    else:
                        pl.when((at >= 0) & (at < A))(functools.partial(body, sg, at))

        def straight(sg, at):
            owner, cid = index(at, b, c), at * B + b
            arrive(owner, 0)
            along(sg, owner, 0, False, cid)
            across(owner, 0, False, at)
            over(owner, 0, False, cid)

            @factors
            def _():
                arrive(owner, 2)
                along(sg, owner, 2, False, cid)
                across(owner, 2, False, A + 1 + at)
                over(owner, 2, False, cid)

        def turned(sg, at):
            for j in range(1, B):
                bb = lax.rem(b + j, B)
                owner, cid = index(at, bb, c), at * B + bb
                arrive(owner, 1)
                along(sg, owner, 1, False, cid)
                over(owner, 1, False, cid)

        def beside(sg, at):
            owner, cid = index(at, b, c), at * B + b
            arrive(owner, 1)
            along(sg, owner, 1, False, cid)
            over(owner, 1, False, cid)

        def crossed(sg, at):
            for j in range(1, B):
                bb = lax.rem(b + j, B)
                owner, cid = index(at, bb, c), at * B + bb
                arrive(owner, 0)
                over(owner, 0, False, cid)

                @factors
                def _():
                    arrive(owner, 2)
                    over(owner, 2, False, cid)

        facing(h, straight)
        facing(h - 1, turned)
        facing(h, beside)
        facing(h - 1, crossed)

    def pass_factors(j):
        return pltpu.make_async_remote_copy(
            src_ref=gt_ref.at[mine],
            dst_ref=gt_ref.at[mine],
            send_sem=tsnd.at[j - 1],
            recv_sem=trcv.at[j - 1],
            device_id={"row": lax.rem(my_row + j, groups)},
            device_id_type=MESH,
        )

    def own_factors():
        return pltpu.make_async_copy(t_ref.at[mine], gt_ref.at[mine, :, me], town)

    def settle(u):
        for at in range(A):
            for bb in range(B):
                for q in range(2):
                    landed(u, index(at, bb, 1 - c), q)

        @pl.when(u == 0)
        def _():
            for at in range(A):
                for bb in range(B):
                    landed(u, index(at, bb, 1 - c), 2)
            own_factors().wait()
            for j in range(1, groups):
                pass_factors(j).start()

    def load(u):
        k, h = panels - 1 - u // H, lax.rem(u, H)
        sl = lax.rem(u, 2 * H)
        pltpu.make_async_copy(v_ref.at[k, h], vbuf.at[sl, me], lsem.at[sl]).start()
        for j in range(1, members):
            owner = lax.rem(me + j, members)
            pltpu.make_async_copy(g_ref.at[k, h, owner], vbuf.at[sl, owner], lsem.at[sl]).start()

    def load_factor(i):
        @pl.when(i == 0)
        def _():
            for j in range(1, groups):
                pass_factors(j).wait_send()
                part = gt_ref.at[pl.ds(lax.rem(my_row + groups - j, groups) * share, share)]
                pltpu.make_async_remote_copy(
                    src_ref=part,
                    dst_ref=part,
                    send_sem=tsnd.at[j - 1],
                    recv_sem=trcv.at[j - 1],
                    device_id={"row": lax.rem(my_row + j, groups)},
                    device_id_type=MESH,
                ).wait_recv()

        return pltpu.make_async_copy(gt_ref.at[panels - 1 - i], tbuf, tlsem).start()

    def partial(sl, j):
        return pltpu.make_async_remote_copy(
            src_ref=psend.at[sl],
            dst_ref=precv.at[sl, j - 1],
            send_sem=psnd.at[sl, j - 1],
            recv_sem=prcv.at[sl, j - 1],
            device_id={"row": lax.rem(my_row + j, groups)},
            device_id_type=MESH,
        )

    def project(u):
        k, h = panels - 1 - u // H, lax.rem(u, H)
        sl = lax.rem(u, 2 * H)
        pltpu.make_async_copy(g_ref.at[k, h], vbuf.at[sl], lsem.at[sl]).wait()
        part = pl.ds(0, members * sub)
        acc[part] = jnp.zeros((members * sub, acc.shape[1]), jnp.float32)

        def body(n, _):
            at = pl.multiple_of(n * tile, tile)
            left = halves(vbuf[sl, :, :, pl.ds(at, tile)].reshape(members * sub, tile))
            right = halves(zbuf[pl.ds(at, tile), :])
            acc[part] += dot3(left, right, 1, 0)
            return 0

        lax.fori_loop(0, rows // tile, body, 0)
        psend[sl] = acc[part]
        for j in range(1, groups):
            partial(sl, j).start()

    def store(n):
        spot = pl.ds(pl.multiple_of(n * tile, tile), tile)
        return pltpu.make_async_copy(zbuf.at[spot], out_ref.at[spot], zsem)

    def update(i, last):
        base = lax.rem(i, 2) * H
        total = []
        for h in range(H):
            whole_sum = psend[base + h]
            for j in range(1, groups):
                partial(base + h, j).wait()
                whole_sum = whole_sum + precv[base + h, j - 1]
            total.append(whole_sum)
        total = halves(jnp.concatenate(total, axis=0))
        pltpu.make_async_copy(gt_ref.at[panels - 1 - i], tbuf, tlsem).wait()
        factor = halves(tbuf[...].reshape(width, width))
        scaled = dot3(factor, total, 0, 0)
        for h in range(H):
            for owner in range(members):
                at = (owner * H + h) * sub
                acc[pl.ds((h * members + owner) * sub, sub), :] = scaled[at : at + sub]
        scaled = halves(acc[...])

        def body(n, _):
            at = pl.multiple_of(n * tile, tile)
            left = halves(vbuf[pl.ds(base, H), :, :, pl.ds(at, tile)].reshape(width, tile))
            zbuf[pl.ds(at, tile), :] = zbuf[pl.ds(at, tile), :] - dot3(left, scaled, 0, 0)
            if last:

                @pl.when(n > 0)
                def _():
                    store(n - 1).start()

            return 0

        lax.fori_loop(0, rows // tile, body, 0)

    fetch = pltpu.make_async_copy(z_hbm, zbuf, zsem)
    fetch.start()
    for u in range(AHEAD):
        hop(jnp.int32(u), 0, True)
    own_factors().start()
    fetch.wait()

    def slot(t, _):
        w = t - A

        @pl.when(w >= 0)
        def _():
            i, h = w // H, lax.rem(w, H)

            @pl.when((h == 0) & (w > 0))
            def _():
                update(i - 1, False)

            @pl.when(h == H - 1)
            def _():
                load_factor(i)

            project(w)

        for h in range(A, 0, -1):
            u = t - (h - 1)

            @pl.when((u >= 0) & (u < units))
            def _(u=u, h=h):
                hop(u, h, True)

        @pl.when(t + AHEAD < units)
        def _():
            hop(t + AHEAD, 0, True)

        v = t - A + 1

        @pl.when((v >= 0) & (v < units))
        def _():
            settle(v)
            load(v)

        @pl.when(w >= 0)
        def _():
            for h in range(A + 1):
                hop(w, h, False)

        return 0

    lax.fori_loop(0, units + A, slot, 0)
    update(jnp.int32(panels - 1), True)
    store(rows // tile - 1).start()
    pltpu.make_async_copy(zbuf, out_ref, zsem).wait()


def local(eigvecs, v_panels, t_panels):
    panels, rows, per = v_panels.shape
    width = t_panels.shape[1]
    groups = lax.axis_size("row")
    members = lax.axis_size("col")
    chips = members // 2
    B = max(n for n in range(1, chips + 1) if chips % n == 0 and n * n <= chips)
    A = chips // B
    columns = eigvecs.shape[1]
    H = per // 8 if per % 8 == 0 else 1
    sub = per // H
    vectors = jnp.transpose(v_panels, (0, 2, 1)).reshape(panels, H, sub, rows)
    factors = jnp.transpose(t_panels, (0, 2, 1)).reshape(panels, H, sub, width)
    dma = pltpu.SemaphoreType.DMA
    anywhere = pl.BlockSpec(memory_space=pl.ANY)
    others = max(groups - 1, 1)
    out, _, _ = pl.pallas_call(
        functools.partial(kernel, (groups, A, B)),
        out_shape=(
            jax.ShapeDtypeStruct((rows, columns), jnp.float32),
            jax.ShapeDtypeStruct((panels, H, members, sub, rows), jnp.float32),
            jax.ShapeDtypeStruct((panels, H, members, sub, width), jnp.float32),
        ),
        in_specs=[anywhere] * 3,
        out_specs=(anywhere,) * 3,
        scratch_shapes=[
            pltpu.VMEM((rows, columns), jnp.float32),
            pltpu.VMEM((2 * H, members, sub, rows), jnp.float32),
            pltpu.VMEM((H, members, sub, width), jnp.float32),
            pltpu.VMEM((width, columns), jnp.float32),
            pltpu.VMEM((2 * H, members * sub, columns), jnp.float32),
            pltpu.VMEM((2 * H, others, members * sub, columns), jnp.float32),
            dma((SLOTS, 3, members)),
            dma((SLOTS, 3, chips)),
            dma((SLOTS, 3, chips)),
            dma((SLOTS, 2 * A + 1, max(B - 1, 1))),
            dma((SLOTS, 3, chips)),
            dma((2 * H,)),
            dma,
            dma((2 * H, others)),
            dma((2 * H, others)),
            dma,
            dma((others,)),
            dma((others,)),
            dma,
        ],
        compiler_params=pltpu.CompilerParams(has_side_effects=True, vmem_limit_bytes=60 * 2**20),
    )(eigvecs, vectors, factors)
    return out


def solution(mesh):
    in_specs = (P("row", "col"), P(None, "row", "col"), P(None, None, "col"))
    out_specs = P("row", "col")
    return jax.shard_map(local, mesh=mesh, in_specs=in_specs, out_specs=out_specs, check_vma=False)
```

```python
import functools

import jax
import jax.numpy as jnp
from jax import lax
from jax.experimental import pallas as pl
from jax.experimental.pallas import tpu as pltpu
from jax.sharding import PartitionSpec as P

SLOTS = 8
AHEAD = 2
MESH = pl.DeviceIdType.MESH


def halves(x):
    high = x.astype(jnp.bfloat16)
    return high, (x - high.astype(jnp.float32)).astype(jnp.bfloat16)


def dot3(left, right, left_axis, right_axis):
    def one(a, b):
        return lax.dot_general(
            a, b, (((left_axis,), (right_axis,)), ((), ())), preferred_element_type=jnp.float32
        )

    (lh, ll), (rh, rl) = left, right
    return one(lh, rh) + (one(ll, rh) + one(lh, rl))


def kernel(shape, z_hbm, v_ref, t_ref, out_ref, zbuf, vbuf, tbuf, acc, psend, precv, *sems):
    groups, A, B = shape
    recv, su, sd, sy, sc, lsem, zsem, psnd, prcv, town, tsnd, trcv = sems
    panels, H, sub, rows = v_ref.shape
    members = 2 * A * B
    ring = vbuf.shape[0]
    width = H * members * sub
    units = panels * H
    share = panels // groups
    tiles = rows // 128
    spare = (B - 1) * A - (A - 1)
    whole = 2 * max((A - 1) * (B - 1), 1)
    side = min(max((tiles * spare + whole // 2) // whole, 1), tiles - 1)
    cut = (tiles - side) * 128
    lanes = (pl.ds(0, cut), pl.ds(cut, rows - cut))
    tile = min(rows, 1024)
    me = lax.axis_index("col")
    my_row = lax.axis_index("row")
    c = lax.rem(me, 2)
    b = lax.rem(me // 2, B)
    a = me // (2 * B)
    mine = pl.ds(my_row * share, share)

    def index(aa, bb, cc):
        return (aa * B + bb) * 2 + cc

    def place(u, owner, q):
        if q == 2:
            return tbuf.at[mine, :, owner]
        return vbuf.at[lax.rem(u // H, ring), lax.rem(u, H), owner, :, lanes[q]]

    def first(u, q):
        if q == 2:
            return t_ref.at[mine]
        return v_ref.at[panels - 1 - u // H, lax.rem(u, H), :, lanes[q]]

    def landed(u, owner, q):
        sl = lax.rem(u, SLOTS)
        spot = place(u, owner, q)
        pltpu.make_async_remote_copy(
            src_ref=spot,
            dst_ref=spot,
            send_sem=sc.at[sl, q, 0],
            recv_sem=recv.at[sl, q, owner],
            device_id={"col": index(a, b, 1 - c)},
            device_id_type=MESH,
        ).wait_recv()

    def hop(u, h, go):
        sl = lax.rem(u, SLOTS)

        def move(owner, q, own, target, sem):
            copy = pltpu.make_async_remote_copy(
                src_ref=first(u, q) if own else place(u, owner, q),
                dst_ref=place(u, owner, q),
                send_sem=sem,
                recv_sem=recv.at[sl, q, owner],
                device_id={"col": target},
                device_id_type=MESH,
            )
            if go:
                copy.start()
            else:
                copy.wait_send()

        def arrive(owner, q):
            if go:
                landed(u, owner, q)

        def along(sg, owner, q, own, cid):
            if sg >= 0:

                @pl.when(a < A - 1)
                def _():
                    move(owner, q, own, index(a + 1, b, c), su.at[sl, q, cid])

            if sg <= 0:

                @pl.when(a > 0)
                def _():
                    move(owner, q, own, index(a - 1, b, c), sd.at[sl, q, cid])

        def across(owner, q, own, slot):
            for j in range(1, B):
                move(owner, q, own, index(a, lax.rem(b + j, B), c), sy.at[sl, slot, j - 1])

        def over(owner, q, own, cid):
            move(owner, q, own, index(a, b, 1 - c), sc.at[sl, q, cid])

        def factors(body):
            pl.when(u == 0)(body)

        def signs(d):
            return (1, -1) if d else (0,)

        if h == 0:
            cid = a * B + b
            if go:
                own_vectors(u).start()
            across(me, 1, True, A)
            along(0, me, 0, True, cid)
            along(0, me, 1, True, cid)
            across(me, 0, True, a)
            over(me, 0, True, cid)
            over(me, 1, True, cid)

            @factors
            def _():
                along(0, me, 2, True, cid)
                across(me, 2, True, A + 1 + a)
                over(me, 2, True, cid)

            return

        def facing(d, body):
            if d < A:
                for sg in signs(d):
                    at = a - sg * d
                    if d == 0:
                        body(sg, at)
                    else:
                        pl.when((at >= 0) & (at < A))(functools.partial(body, sg, at))

        def straight(sg, at):
            owner, cid = index(at, b, c), at * B + b
            arrive(owner, 0)
            along(sg, owner, 0, False, cid)
            across(owner, 0, False, at)
            over(owner, 0, False, cid)

            @factors
            def _():
                arrive(owner, 2)
                along(sg, owner, 2, False, cid)
                across(owner, 2, False, A + 1 + at)
                over(owner, 2, False, cid)

        def turned(sg, at):
            for j in range(1, B):
                bb = lax.rem(b + j, B)
                owner, cid = index(at, bb, c), at * B + bb
                arrive(owner, 1)
                along(sg, owner, 1, False, cid)
                over(owner, 1, False, cid)

        def beside(sg, at):
            owner, cid = index(at, b, c), at * B + b
            arrive(owner, 1)
            along(sg, owner, 1, False, cid)
            over(owner, 1, False, cid)

        def crossed(sg, at):
            for j in range(1, B):
                bb = lax.rem(b + j, B)
                owner, cid = index(at, bb, c), at * B + bb
                arrive(owner, 0)
                over(owner, 0, False, cid)

                @factors
                def _():
                    arrive(owner, 2)
                    over(owner, 2, False, cid)

        facing(h, straight)
        facing(h - 1, turned)
        facing(h, beside)
        facing(h - 1, crossed)

    def pass_factors(j):
        return pltpu.make_async_remote_copy(
            src_ref=tbuf.at[mine],
            dst_ref=tbuf.at[mine],
            send_sem=tsnd.at[j - 1],
            recv_sem=trcv.at[j - 1],
            device_id={"row": lax.rem(my_row + j, groups)},
            device_id_type=MESH,
        )

    def own_factors():
        return pltpu.make_async_copy(t_ref.at[mine], tbuf.at[mine, :, me], town)

    def settle(u):
        for at in range(A):
            for bb in range(B):
                for q in range(2):
                    landed(u, index(at, bb, 1 - c), q)

        @pl.when(u == 0)
        def _():
            for at in range(A):
                for bb in range(B):
                    landed(u, index(at, bb, 1 - c), 2)
            own_factors().wait()
            for j in range(1, groups):
                pass_factors(j).start()

    def own_vectors(u):
        return pltpu.make_async_copy(
            v_ref.at[panels - 1 - u // H, lax.rem(u, H)],
            vbuf.at[lax.rem(u // H, ring), lax.rem(u, H), me],
            lsem.at[lax.rem(u, SLOTS)],
        )

    def swap_factors():
        for j in range(1, groups):
            pass_factors(j).wait_send()
            part = tbuf.at[pl.ds(lax.rem(my_row + groups - j, groups) * share, share)]
            pltpu.make_async_remote_copy(
                src_ref=part,
                dst_ref=part,
                send_sem=tsnd.at[j - 1],
                recv_sem=trcv.at[j - 1],
                device_id={"row": lax.rem(my_row + j, groups)},
                device_id_type=MESH,
            ).wait_recv()

    def partial(sl, j):
        return pltpu.make_async_remote_copy(
            src_ref=psend.at[sl],
            dst_ref=precv.at[sl, j - 1],
            send_sem=psnd.at[sl, j - 1],
            recv_sem=prcv.at[sl, j - 1],
            device_id={"row": lax.rem(my_row + j, groups)},
            device_id_type=MESH,
        )

    def project(u):
        spot, h = lax.rem(u // H, ring), lax.rem(u, H)
        sl = lax.rem(u, 2 * H)
        own_vectors(u).wait()
        part = pl.ds(0, members * sub)
        acc[part] = jnp.zeros((members * sub, acc.shape[1]), jnp.float32)

        def body(n, _):
            at = pl.multiple_of(n * tile, tile)
            left = halves(vbuf[spot, h, :, :, pl.ds(at, tile)].reshape(members * sub, tile))
            right = halves(zbuf[pl.ds(at, tile), :])
            acc[part] += dot3(left, right, 1, 0)
            return 0

        lax.fori_loop(0, rows // tile, body, 0)
        psend[sl] = acc[part]
        for j in range(1, groups):
            partial(sl, j).start()

    def store(n):
        spot = pl.ds(pl.multiple_of(n * tile, tile), tile)
        return pltpu.make_async_copy(zbuf.at[spot], out_ref.at[spot], zsem)

    def update(i, last):
        base = lax.rem(i, 2) * H
        total = []
        for h in range(H):
            whole_sum = psend[base + h]
            for j in range(1, groups):
                partial(base + h, j).wait()
                whole_sum = whole_sum + precv[base + h, j - 1]
            total.append(whole_sum)
        total = halves(jnp.concatenate(total, axis=0))
        spot = lax.rem(i, ring)
        factor = halves(tbuf[panels - 1 - i].reshape(width, width))
        scaled = dot3(factor, total, 0, 0)
        for h in range(H):
            for owner in range(members):
                at = (owner * H + h) * sub
                acc[pl.ds((h * members + owner) * sub, sub), :] = scaled[at : at + sub]
        scaled = halves(acc[...])

        def body(n, _):
            at = pl.multiple_of(n * tile, tile)
            left = halves(vbuf[spot, :, :, :, pl.ds(at, tile)].reshape(width, tile))
            zbuf[pl.ds(at, tile), :] = zbuf[pl.ds(at, tile), :] - dot3(left, scaled, 0, 0)
            if last:

                @pl.when(n > 0)
                def _():
                    store(n - 1).start()

            return 0

        lax.fori_loop(0, rows // tile, body, 0)

    fetch = pltpu.make_async_copy(z_hbm, zbuf, zsem)
    fetch.start()
    for u in range(AHEAD):
        hop(jnp.int32(u), 0, True)
    own_factors().start()
    fetch.wait()

    def slot(t, _):
        w = t - A

        @pl.when(w >= 0)
        def _():
            i, h = w // H, lax.rem(w, H)

            @pl.when((h == 0) & (i == 1))
            def _():
                swap_factors()

            @pl.when((h == 0) & (w > 0))
            def _():
                update(i - 1, False)

            project(w)

        for h in range(A, 0, -1):
            u = t - (h - 1)

            @pl.when((u >= 0) & (u < units))
            def _(u=u, h=h):
                hop(u, h, True)

        @pl.when(t + AHEAD < units)
        def _():
            hop(t + AHEAD, 0, True)

        v = t - A + 1

        @pl.when((v >= 0) & (v < units))
        def _():
            settle(v)

        @pl.when(w >= 0)
        def _():
            for h in range(A + 1):
                hop(w, h, False)

        return 0

    lax.fori_loop(0, units + A, slot, 0)
    update(jnp.int32(panels - 1), True)
    store(rows // tile - 1).start()
    pltpu.make_async_copy(zbuf, out_ref, zsem).wait()


def local(eigvecs, v_panels, t_panels):
    panels, rows, per = v_panels.shape
    width = t_panels.shape[1]
    groups = lax.axis_size("row")
    members = lax.axis_size("col")
    chips = members // 2
    B = max(n for n in range(1, chips + 1) if chips % n == 0 and n * n <= chips)
    A = chips // B
    columns = eigvecs.shape[1]
    H = per // 8 if per % 8 == 0 else 1
    sub = per // H
    vectors = jnp.transpose(v_panels, (0, 2, 1)).reshape(panels, H, sub, rows)
    factors = jnp.transpose(t_panels, (0, 2, 1)).reshape(panels, H, sub, width)
    dma = pltpu.SemaphoreType.DMA
    anywhere = pl.BlockSpec(memory_space=pl.ANY)
    others = max(groups - 1, 1)
    ring = min(panels, 1 + (A + AHEAD + 2 + H - 1) // H)
    out = pl.pallas_call(
        functools.partial(kernel, (groups, A, B)),
        out_shape=jax.ShapeDtypeStruct((rows, columns), jnp.float32),
        in_specs=[anywhere] * 3,
        out_specs=anywhere,
        scratch_shapes=[
            pltpu.VMEM((rows, columns), jnp.float32),
            pltpu.VMEM((ring, H, members, sub, rows), jnp.float32),
            pltpu.VMEM((panels, H, members, sub, width), jnp.float32),
            pltpu.VMEM((width, columns), jnp.float32),
            pltpu.VMEM((2 * H, members * sub, columns), jnp.float32),
            pltpu.VMEM((2 * H, others, members * sub, columns), jnp.float32),
            dma((SLOTS, 3, members)),
            dma((SLOTS, 3, chips)),
            dma((SLOTS, 3, chips)),
            dma((SLOTS, 2 * A + 1, max(B - 1, 1))),
            dma((SLOTS, 3, chips)),
            dma((SLOTS,)),
            dma,
            dma((2 * H, others)),
            dma((2 * H, others)),
            dma,
            dma((others,)),
            dma((others,)),
        ],
        compiler_params=pltpu.CompilerParams(has_side_effects=True, vmem_limit_bytes=54 * 2**20),
    )(eigvecs, vectors, factors)
    return out


def solution(mesh):
    in_specs = (P("row", "col"), P(None, "row", "col"), P(None, None, "col"))
    out_specs = P("row", "col")
    return jax.shard_map(local, mesh=mesh, in_specs=in_specs, out_specs=out_specs, check_vma=False)
```

```python
import functools

import jax
import jax.numpy as jnp
from jax import lax
from jax.experimental import pallas as pl
from jax.experimental.pallas import tpu as pltpu
from jax.sharding import PartitionSpec as P

SLOTS = 8
AHEAD = 2
MESH = pl.DeviceIdType.MESH


def halves(x):
    high = x.astype(jnp.bfloat16)
    return high, (x - high.astype(jnp.float32)).astype(jnp.bfloat16)


def dot3(left, right, left_axis, right_axis):
    def one(a, b):
        return lax.dot_general(
            a, b, (((left_axis,), (right_axis,)), ((), ())), preferred_element_type=jnp.float32
        )

    (lh, ll), (rh, rl) = left, right
    return one(lh, rh) + (one(ll, rh) + one(lh, rl))


def kernel(shape, z_hbm, v_ref, t_ref, out_ref, zbuf, vbuf, tbuf, stage, acc, psend, precv, *sems):
    groups, A, B, zone, tile = shape
    recv, su, sd, sy, sc, lsem, zsem, psnd, prcv, town, tsnd, trcv = sems[:12]
    lsnd, lrcv, gsnd, grcv = sems[12:]
    panels, H, sub, rows = v_ref.shape
    members = 2 * A * B
    ring = vbuf.shape[0]
    width = H * members * sub
    units = panels * H
    share = panels // groups
    tiles = rows // 128
    spare = (B - 1) * A - (A - 1)
    whole = 2 * max((A - 1) * (B - 1), 1)
    side = min(max((tiles * spare + whole // 2) // whole, 1), tiles - 1)
    cut = (tiles - side) * 128
    half = zone // 2
    floor = zone // width
    early = (panels - floor) * H if zone else 0
    lanes = (pl.ds(half, cut - half), pl.ds(cut, rows - cut), None, pl.ds(0, half))
    me = lax.axis_index("col")
    my_row = lax.axis_index("row")
    c = lax.rem(me, 2)
    b = lax.rem(me // 2, B)
    a = me // (2 * B)
    mine = pl.ds(my_row * share, share)

    def index(aa, bb, cc):
        return (aa * B + bb) * 2 + cc

    def place(u, owner, q):
        if q == 2:
            return tbuf.at[mine, :, owner]
        return vbuf.at[lax.rem(u // H, ring), lax.rem(u, H), owner, :, lanes[q]]

    def source(u, span):
        return v_ref.at[panels - 1 - u // H, lax.rem(u, H), :, span]

    def slot_of(u, span):
        return vbuf.at[lax.rem(u // H, ring), lax.rem(u, H), me, :, span]

    def staged(u):
        return stage.at[panels - 1 - u // H - floor, lax.rem(u, H)]

    low, mid, high = pl.ds(0, half), pl.ds(half, zone - half), pl.ds(zone, rows - zone)

    def lent(u, body):
        if zone:
            borrowed = (my_row == 0) & (u < early)
            pl.when(borrowed)(lambda: body(staged(u)))
            pl.when(jnp.logical_not(borrowed))(lambda: body(source(u, mid)))

    def landed(u, owner, q):
        sl = lax.rem(u, SLOTS)
        spot = place(u, owner, q)
        pltpu.make_async_remote_copy(
            src_ref=spot,
            dst_ref=spot,
            send_sem=sc.at[sl, q, 0],
            recv_sem=recv.at[sl, q, owner],
            device_id={"col": index(a, b, 1 - c)},
            device_id_type=MESH,
        ).wait_recv()

    def hop(u, h, go, stages=(0, 1)):
        sl = lax.rem(u, SLOTS)

        def move(owner, q, own, target, sem, part=None):
            def copy(src, dst):
                return pltpu.make_async_remote_copy(
                    src_ref=src,
                    dst_ref=dst,
                    send_sem=sem,
                    recv_sem=recv.at[sl, q, owner],
                    device_id={"col": target},
                    device_id_type=MESH,
                )

            spot = place(u, owner, q)
            if not go:
                copy(spot, spot).wait_send()
            elif not own:
                copy(spot, spot).start()
            elif part == "mid":
                lent(u, lambda src: copy(src, slot_of(u, mid)).start())
            elif q == 2:
                copy(t_ref.at[mine], spot).start()
            elif q == 0:
                span = pl.ds(zone, cut - zone)
                copy(source(u, span), slot_of(u, span)).start()
            else:
                copy(source(u, lanes[q]), spot).start()

        def arrive(owner, q):
            if go:
                landed(u, owner, q)

        def along(sg, owner, q, own, cid, part=None):
            if sg >= 0:

                @pl.when(a < A - 1)
                def _():
                    move(owner, q, own, index(a + 1, b, c), su.at[sl, q, cid], part)

            if sg <= 0:

                @pl.when(a > 0)
                def _():
                    move(owner, q, own, index(a - 1, b, c), sd.at[sl, q, cid], part)

        def across(owner, q, own, at, part=None):
            slot = (at, A, A + 1 + at, 2 * A + 1 + at)[q]
            for j in range(1, B):
                move(owner, q, own, index(a, lax.rem(b + j, B), c), sy.at[sl, slot, j - 1], part)

        def over(owner, q, own, cid, part=None):
            move(owner, q, own, index(a, b, 1 - c), sc.at[sl, q, cid], part)

        def extras(body):
            pl.when(u == 0)(functools.partial(body, 2))
            if zone:
                pl.when(u >= early)(functools.partial(body, 3))

        def signs(d):
            return (1, -1) if d else (0,)

        def spread(q, part=None):
            cid = a * B + b
            along(0, me, q, True, cid, part)
            across(me, q, True, a, part)
            over(me, q, True, cid, part)

        if h == 0:
            if 0 in stages:
                across(me, 1, True, a)
                along(0, me, 0, True, a * B + b)
                along(0, me, 1, True, a * B + b)
                across(me, 0, True, a)
                over(me, 0, True, a * B + b)
                over(me, 1, True, a * B + b)
                extras(spread)
            if 1 in stages and go:
                if zone:
                    spread(0, "mid")
                own_vectors(u)
            return

        def facing(d, body):
            if d < A:
                for sg in signs(d):
                    at = a - sg * d
                    if d == 0:
                        body(sg, at)
                    else:
                        pl.when((at >= 0) & (at < A))(functools.partial(body, sg, at))

        def straight(sg, at):
            owner, cid = index(at, b, c), at * B + b
            arrive(owner, 0)
            along(sg, owner, 0, False, cid)
            across(owner, 0, False, at)
            over(owner, 0, False, cid)

            @extras
            def _(q):
                arrive(owner, q)
                along(sg, owner, q, False, cid)
                across(owner, q, False, at)
                over(owner, q, False, cid)

        def turned(sg, at):
            for j in range(1, B):
                bb = lax.rem(b + j, B)
                owner, cid = index(at, bb, c), at * B + bb
                arrive(owner, 1)
                along(sg, owner, 1, False, cid)
                over(owner, 1, False, cid)

        def beside(sg, at):
            owner, cid = index(at, b, c), at * B + b
            arrive(owner, 1)
            along(sg, owner, 1, False, cid)
            over(owner, 1, False, cid)

        def crossed(sg, at):
            for j in range(1, B):
                bb = lax.rem(b + j, B)
                owner, cid = index(at, bb, c), at * B + bb
                arrive(owner, 0)
                over(owner, 0, False, cid)

                @extras
                def _(q):
                    arrive(owner, q)
                    over(owner, q, False, cid)

        facing(h, straight)
        facing(h - 1, turned)
        facing(h, beside)
        facing(h - 1, crossed)

    def pass_factors(j):
        return pltpu.make_async_remote_copy(
            src_ref=tbuf.at[mine],
            dst_ref=tbuf.at[mine],
            send_sem=tsnd.at[j - 1],
            recv_sem=trcv.at[j - 1],
            device_id={"row": lax.rem(my_row + j, groups)},
            device_id_type=MESH,
        )

    def own_factors():
        return pltpu.make_async_copy(t_ref.at[mine], tbuf.at[mine, :, me], town)

    def settle(u):
        for at in range(A):
            for bb in range(B):
                for q in range(2):
                    landed(u, index(at, bb, 1 - c), q)

        if zone:

            @pl.when(u >= early)
            def _():
                for at in range(A):
                    for bb in range(B):
                        landed(u, index(at, bb, 1 - c), 3)
                own_arrived(u, pl.ds(0, rows))

            @pl.when(u < early)
            def _():
                own_arrived(u, pl.ds(half, rows - half))

                @pl.when(my_row == 0)
                def _():
                    hand(u).start()
        else:
            own_arrived(u, pl.ds(0, rows))

        @pl.when(u == 0)
        def _():
            for at in range(A):
                for bb in range(B):
                    landed(u, index(at, bb, 1 - c), 2)
            own_factors().wait()
            for j in range(1, groups):
                pass_factors(j).start()

    def own_vectors(u):
        sem = lsem.at[lax.rem(u, SLOTS)]
        pltpu.make_async_copy(source(u, high), slot_of(u, high), sem).start()
        if zone:
            lent(u, lambda src: pltpu.make_async_copy(src, slot_of(u, mid), sem).start())

            @pl.when(u >= early)
            def _():
                pltpu.make_async_copy(source(u, low), slot_of(u, low), sem).start()

    def own_arrived(u, span):
        pltpu.make_async_copy(source(u, span), slot_of(u, span), lsem.at[lax.rem(u, SLOTS)]).wait()

    def lend():
        return pltpu.make_async_remote_copy(
            src_ref=v_ref.at[pl.ds(floor, panels - floor), :, :, low],
            dst_ref=stage,
            send_sem=lsnd,
            recv_sem=lrcv,
            device_id={"row": 1 - my_row},
            device_id_type=MESH,
        )

    def hand(u):
        spot, h = lax.rem(u // H, ring), lax.rem(u, H)
        return pltpu.make_async_remote_copy(
            src_ref=vbuf.at[spot, h, :, :, mid],
            dst_ref=vbuf.at[spot, h, :, :, low],
            send_sem=gsnd.at[lax.rem(u, SLOTS)],
            recv_sem=grcv.at[lax.rem(u, SLOTS)],
            device_id={"row": 1 - my_row},
            device_id_type=MESH,
        )

    def begin(u):
        return jnp.where((my_row == 0) & (u < early), 1, 0) if zone else 0

    def swap_factors():
        for j in range(1, groups):
            pass_factors(j).wait_send()
            part = tbuf.at[pl.ds(lax.rem(my_row + groups - j, groups) * share, share)]
            pltpu.make_async_remote_copy(
                src_ref=part,
                dst_ref=part,
                send_sem=tsnd.at[j - 1],
                recv_sem=trcv.at[j - 1],
                device_id={"row": lax.rem(my_row + j, groups)},
                device_id_type=MESH,
            ).wait_recv()

    def partial(sl, j):
        return pltpu.make_async_remote_copy(
            src_ref=psend.at[sl],
            dst_ref=precv.at[sl, j - 1],
            send_sem=psnd.at[sl, j - 1],
            recv_sem=prcv.at[sl, j - 1],
            device_id={"row": lax.rem(my_row + j, groups)},
            device_id_type=MESH,
        )

    def project(u):
        spot, h = lax.rem(u // H, ring), lax.rem(u, H)
        sl = lax.rem(u, 2 * H)
        if zone:

            @pl.when((my_row == 1) & (u < early))
            def _():
                hand(u).wait_recv()

        part = pl.ds(0, members * sub)
        acc[part] = jnp.zeros((members * sub, acc.shape[1]), jnp.float32)

        def body(n, _):
            at = pl.multiple_of(n * tile, tile)
            left = halves(vbuf[spot, h, :, :, pl.ds(at, tile)].reshape(members * sub, tile))
            right = halves(zbuf[pl.ds(at, tile), :])
            acc[part] += dot3(left, right, 1, 0)
            return 0

        lax.fori_loop(begin(u), rows // tile, body, 0)
        psend[sl] = acc[part]
        for j in range(1, groups):
            partial(sl, j).start()

    def store(n):
        spot = pl.ds(pl.multiple_of(n * tile, tile), tile)
        return pltpu.make_async_copy(zbuf.at[spot], out_ref.at[spot], zsem)

    def update(i, last):
        base = lax.rem(i, 2) * H
        total = []
        for h in range(H):
            whole_sum = psend[base + h]
            for j in range(1, groups):
                partial(base + h, j).wait()
                whole_sum = whole_sum + precv[base + h, j - 1]
            total.append(whole_sum)
        total = halves(jnp.concatenate(total, axis=0))
        spot = lax.rem(i, ring)
        factor = halves(tbuf[panels - 1 - i].reshape(width, width))
        scaled = dot3(factor, total, 0, 0)
        for h in range(H):
            for owner in range(members):
                at = (owner * H + h) * sub
                acc[pl.ds((h * members + owner) * sub, sub), :] = scaled[at : at + sub]
        scaled = halves(acc[...])

        def body(n, _):
            at = pl.multiple_of(n * tile, tile)
            left = halves(vbuf[spot, :, :, :, pl.ds(at, tile)].reshape(width, tile))
            zbuf[pl.ds(at, tile), :] = zbuf[pl.ds(at, tile), :] - dot3(left, scaled, 0, 0)
            if last:

                @pl.when(n > 0)
                def _():
                    store(n - 1).start()

            return 0

        lax.fori_loop(0 if last else begin(i * H), rows // tile, body, 0)

    fetch = pltpu.make_async_copy(z_hbm, zbuf, zsem)
    if zone:

        @pl.when(my_row == 1)
        def _():
            lend().start()

    for u in range(AHEAD):
        hop(jnp.int32(u), 0, True, (0,))
    fetch.start()
    own_factors().start()
    if zone:

        @pl.when(my_row == 0)
        def _():
            lend().wait_recv()

    for u in range(AHEAD):
        hop(jnp.int32(u), 0, True, (1,))
    fetch.wait()

    def slot(t, _):
        w = t - A

        @pl.when(w >= 0)
        def _():
            i, h = w // H, lax.rem(w, H)

            @pl.when((h == 0) & (i == 1))
            def _():
                swap_factors()

            @pl.when((h == 0) & (w > 0))
            def _():
                update(i - 1, False)

            project(w)

        for h in range(A, 0, -1):
            u = t - (h - 1)

            @pl.when((u >= 0) & (u < units))
            def _(u=u, h=h):
                hop(u, h, True)

        @pl.when(t + AHEAD < units)
        def _():
            hop(t + AHEAD, 0, True)

        v = t - A + 1

        @pl.when((v >= 0) & (v < units))
        def _():
            settle(v)

        @pl.when(w >= 0)
        def _():
            for h in range(A + 1):
                hop(w, h, False)
            if zone:

                @pl.when((my_row == 0) & (w < early))
                def _():
                    hand(w).wait_send()

        return 0

    lax.fori_loop(0, units + A, slot, 0)
    update(jnp.int32(panels - 1), True)
    if zone:

        @pl.when(my_row == 1)
        def _():
            lend().wait_send()

    store(rows // tile - 1).start()
    pltpu.make_async_copy(zbuf, out_ref, zsem).wait()


def local(eigvecs, v_panels, t_panels):
    panels, rows, per = v_panels.shape
    width = t_panels.shape[1]
    groups = lax.axis_size("row")
    members = lax.axis_size("col")
    chips = members // 2
    B = max(n for n in range(1, chips + 1) if chips % n == 0 and n * n <= chips)
    A = chips // B
    columns = eigvecs.shape[1]
    H = per // 8 if per % 8 == 0 else 1
    sub = per // H
    vectors = jnp.transpose(v_panels, (0, 2, 1)).reshape(panels, H, sub, rows)
    factors = jnp.transpose(t_panels, (0, 2, 1)).reshape(panels, H, sub, width)
    dma = pltpu.SemaphoreType.DMA
    anywhere = pl.BlockSpec(memory_space=pl.ANY)
    others = max(groups - 1, 1)
    ring = min(panels, 1 + (A + AHEAD + 2 + H - 1) // H)
    tile = min(rows, 1024)
    zone = tile if groups == 2 and rows >= 4 * tile and tile % (2 * width) == 0 and tile < panels * width else 0
    lent = (panels - zone // width, H, sub, zone // 2) if zone else (1, H, sub, 128)
    out = pl.pallas_call(
        functools.partial(kernel, (groups, A, B, zone, tile)),
        out_shape=jax.ShapeDtypeStruct((rows, columns), jnp.float32),
        in_specs=[anywhere] * 3,
        out_specs=anywhere,
        scratch_shapes=[
            pltpu.VMEM((rows, columns), jnp.float32),
            pltpu.VMEM((ring, H, members, sub, rows), jnp.float32),
            pltpu.VMEM((panels, H, members, sub, width), jnp.float32),
            pltpu.VMEM(lent, jnp.float32),
            pltpu.VMEM((width, columns), jnp.float32),
            pltpu.VMEM((2 * H, members * sub, columns), jnp.float32),
            pltpu.VMEM((2 * H, others, members * sub, columns), jnp.float32),
            dma((SLOTS, 4, members)),
            dma((SLOTS, 4, chips)),
            dma((SLOTS, 4, chips)),
            dma((SLOTS, 3 * A + 1, max(B - 1, 1))),
            dma((SLOTS, 4, chips)),
            dma((SLOTS,)),
            dma,
            dma((2 * H, others)),
            dma((2 * H, others)),
            dma,
            dma((others,)),
            dma((others,)),
            dma,
            dma,
            dma((SLOTS,)),
            dma((SLOTS,)),
        ],
        compiler_params=pltpu.CompilerParams(has_side_effects=True, vmem_limit_bytes=54 * 2**20),
    )(eigvecs, vectors, factors)
    return out


def solution(mesh):
    in_specs = (P("row", "col"), P(None, "row", "col"), P(None, None, "col"))
    out_specs = P("row", "col")
    return jax.shard_map(local, mesh=mesh, in_specs=in_specs, out_specs=out_specs, check_vma=False)
```

```python
import functools

import jax
import jax.numpy as jnp
from jax import lax
from jax.experimental import pallas as pl
from jax.experimental.pallas import tpu as pltpu
from jax.sharding import PartitionSpec as P

SLOTS = 8
AHEAD = 2
MESH = pl.DeviceIdType.MESH


def halves(x):
    high = x.astype(jnp.bfloat16)
    return high, (x - high.astype(jnp.float32)).astype(jnp.bfloat16)


def dot3(left, right, left_axis, right_axis):
    def one(a, b):
        return lax.dot_general(
            a, b, (((left_axis,), (right_axis,)), ((), ())), preferred_element_type=jnp.float32
        )

    (lh, ll), (rh, rl) = left, right
    return one(lh, rh) + (one(ll, rh) + one(lh, rl))


def kernel(shape, z_hbm, v_ref, t_ref, out_ref, zbuf, vbuf, tbuf, stage, acc, psend, precv, *sems):
    groups, A, B, zone, tile = shape
    recv, su, sd, sy, sc, lsem, zsem, psnd, prcv, town, tsnd, trcv = sems[:12]
    lsnd, lrcv, gsnd, grcv = sems[12:]
    panels, H, sub, rows = v_ref.shape
    members = 2 * A * B
    ring = vbuf.shape[0]
    width = H * members * sub
    units = panels * H
    share = panels // groups
    tiles = rows // 128
    spare = (B - 1) * A - (A - 1)
    whole = 2 * max((A - 1) * (B - 1), 1)
    side = min(max((tiles * spare + whole // 2) // whole, 1), tiles - 1)
    cut = (tiles - side) * 128
    half = zone // 2
    floor = zone // width
    early = (panels - floor) * H if zone else 0
    me = lax.axis_index("col")
    my_row = lax.axis_index("row")
    c = lax.rem(me, 2)
    b = lax.rem(me // 2, B)
    a = me // (2 * B)
    mine = pl.ds(my_row * share, share)

    def index(aa, bb, cc):
        return (aa * B + bb) * 2 + cc

    def place(u, owner, q, start=0):
        if q == 2:
            return tbuf.at[mine, :, owner]
        span = pl.ds(cut, rows - cut) if q else pl.ds(start, cut - start)
        return vbuf.at[lax.rem(u // H, ring), lax.rem(u, H), owner, :, span]

    def sized(u, q, body):
        if zone and q == 0:
            pl.when(u < early)(lambda: body(half))
            pl.when(u >= early)(lambda: body(0))
        else:
            body(0)

    def source(u, span):
        return v_ref.at[panels - 1 - u // H, lax.rem(u, H), :, span]

    def slot_of(u, span):
        return vbuf.at[lax.rem(u // H, ring), lax.rem(u, H), me, :, span]

    def staged(u):
        return stage.at[panels - 1 - u // H - floor, lax.rem(u, H)]

    low, mid, high = pl.ds(0, half), pl.ds(half, zone - half), pl.ds(zone, rows - zone)

    def lent(u, body):
        borrowed = (my_row == 0) & (u < early)
        pl.when(borrowed)(lambda: body(staged(u)))

    def landed(u, owner, q):
        sl = lax.rem(u, SLOTS)

        def wait(start):
            spot = place(u, owner, q, start)
            pltpu.make_async_remote_copy(
                src_ref=spot,
                dst_ref=spot,
                send_sem=sc.at[sl, q, 0],
                recv_sem=recv.at[sl, q, owner],
                device_id={"col": index(a, b, 1 - c)},
                device_id_type=MESH,
            ).wait_recv()

        sized(u, q, wait)

    def hop(u, h, go, stages=(0, 1)):
        sl = lax.rem(u, SLOTS)

        def move(owner, q, own, target, sem, part=None):
            def copy(src, dst):
                return pltpu.make_async_remote_copy(
                    src_ref=src,
                    dst_ref=dst,
                    send_sem=sem,
                    recv_sem=recv.at[sl, q, owner],
                    device_id={"col": target},
                    device_id_type=MESH,
                )

            def whole(start):
                spot = place(u, owner, q, start)
                if not go:
                    copy(spot, spot).wait_send()
                elif q == 2 and own:
                    copy(t_ref.at[mine], spot).start()
                elif own:
                    span = pl.ds(cut, rows - cut) if q else pl.ds(start, cut - start)
                    copy(source(u, span), spot).start()
                else:
                    copy(spot, spot).start()

            if part == "mid":
                lent(u, lambda src: copy(src, slot_of(u, mid)).start())
            elif zone and go and own and q == 0:
                borrowed = (my_row == 0) & (u < early)
                pl.when(borrowed)(lambda: whole(zone))
                pl.when(jnp.logical_not(borrowed) & (u < early))(lambda: whole(half))
                pl.when(u >= early)(lambda: whole(0))
            else:
                sized(u, q, whole)

        def arrive(owner, q):
            if go:
                landed(u, owner, q)

        def along(sg, owner, q, own, cid, part=None):
            if sg >= 0:

                @pl.when(a < A - 1)
                def _():
                    move(owner, q, own, index(a + 1, b, c), su.at[sl, q, cid], part)

            if sg <= 0:

                @pl.when(a > 0)
                def _():
                    move(owner, q, own, index(a - 1, b, c), sd.at[sl, q, cid], part)

        def across(owner, q, own, at, part=None):
            slot = (at, A, A + 1 + at)[q]
            for j in range(1, B):
                move(owner, q, own, index(a, lax.rem(b + j, B), c), sy.at[sl, slot, j - 1], part)

        def over(owner, q, own, cid, part=None):
            move(owner, q, own, index(a, b, 1 - c), sc.at[sl, q, cid], part)

        def factors(body):
            pl.when(u == 0)(body)

        def signs(d):
            return (1, -1) if d else (0,)

        def spread(q, part=None):
            cid = a * B + b
            along(0, me, q, True, cid, part)
            across(me, q, True, a, part)
            over(me, q, True, cid, part)

        if h == 0:
            if 0 in stages:
                across(me, 1, True, a)
                along(0, me, 0, True, a * B + b)
                along(0, me, 1, True, a * B + b)
                across(me, 0, True, a)
                over(me, 0, True, a * B + b)
                over(me, 1, True, a * B + b)
                factors(lambda: spread(2))
            if 1 in stages and go:
                if zone:
                    spread(0, "mid")
                own_vectors(u)
            return

        def facing(d, body):
            if d < A:
                for sg in signs(d):
                    at = a - sg * d
                    if d == 0:
                        body(sg, at)
                    else:
                        pl.when((at >= 0) & (at < A))(functools.partial(body, sg, at))

        def straight(sg, at):
            owner, cid = index(at, b, c), at * B + b
            arrive(owner, 0)
            along(sg, owner, 0, False, cid)
            across(owner, 0, False, at)
            over(owner, 0, False, cid)

            @factors
            def _():
                arrive(owner, 2)
                along(sg, owner, 2, False, cid)
                across(owner, 2, False, at)
                over(owner, 2, False, cid)

        def turned(sg, at):
            for j in range(1, B):
                bb = lax.rem(b + j, B)
                owner, cid = index(at, bb, c), at * B + bb
                arrive(owner, 1)
                along(sg, owner, 1, False, cid)
                over(owner, 1, False, cid)

        def beside(sg, at):
            owner, cid = index(at, b, c), at * B + b
            arrive(owner, 1)
            along(sg, owner, 1, False, cid)
            over(owner, 1, False, cid)

        def crossed(sg, at):
            for j in range(1, B):
                bb = lax.rem(b + j, B)
                owner, cid = index(at, bb, c), at * B + bb
                arrive(owner, 0)
                over(owner, 0, False, cid)

                @factors
                def _():
                    arrive(owner, 2)
                    over(owner, 2, False, cid)

        facing(h, straight)
        facing(h - 1, turned)
        facing(h, beside)
        facing(h - 1, crossed)

    def pass_factors(j):
        return pltpu.make_async_remote_copy(
            src_ref=tbuf.at[mine],
            dst_ref=tbuf.at[mine],
            send_sem=tsnd.at[j - 1],
            recv_sem=trcv.at[j - 1],
            device_id={"row": lax.rem(my_row + j, groups)},
            device_id_type=MESH,
        )

    def own_factors():
        return pltpu.make_async_copy(t_ref.at[mine], tbuf.at[mine, :, me], town)

    def settle(u):
        for at in range(A):
            for bb in range(B):
                for q in range(2):
                    landed(u, index(at, bb, 1 - c), q)

        if zone:

            @pl.when(u >= early)
            def _():
                own_arrived(u, pl.ds(0, rows))

            @pl.when(u < early)
            def _():
                own_arrived(u, pl.ds(half, rows - half))

                @pl.when(my_row == 0)
                def _():
                    hand(u).start()
        else:
            own_arrived(u, pl.ds(0, rows))

        @pl.when(u == 0)
        def _():
            for at in range(A):
                for bb in range(B):
                    landed(u, index(at, bb, 1 - c), 2)
            own_factors().wait()
            for j in range(1, groups):
                pass_factors(j).start()

    def own_vectors(u):
        def fetch_own(src, span):
            pltpu.make_async_copy(src, slot_of(u, span), lsem.at[lax.rem(u, SLOTS)]).start()

        if zone:
            lent(u, lambda src: fetch_own(src, mid))
            rest = pl.ds(half, rows - half)
            borrowed = (my_row == 0) & (u < early)
            pl.when(borrowed)(lambda: fetch_own(source(u, high), high))
            pl.when(jnp.logical_not(borrowed) & (u < early))(lambda: fetch_own(source(u, rest), rest))
            pl.when(u >= early)(lambda: fetch_own(source(u, pl.ds(0, rows)), pl.ds(0, rows)))
        else:
            fetch_own(source(u, pl.ds(0, rows)), pl.ds(0, rows))

    def own_arrived(u, span):
        pltpu.make_async_copy(source(u, span), slot_of(u, span), lsem.at[lax.rem(u, SLOTS)]).wait()

    def lend():
        return pltpu.make_async_remote_copy(
            src_ref=v_ref.at[pl.ds(floor, panels - floor), :, :, low],
            dst_ref=stage,
            send_sem=lsnd,
            recv_sem=lrcv,
            device_id={"row": 1 - my_row},
            device_id_type=MESH,
        )

    def hand(u):
        spot, h = lax.rem(u // H, ring), lax.rem(u, H)
        return pltpu.make_async_remote_copy(
            src_ref=vbuf.at[spot, h, :, :, mid],
            dst_ref=vbuf.at[spot, h, :, :, low],
            send_sem=gsnd.at[lax.rem(u, SLOTS)],
            recv_sem=grcv.at[lax.rem(u, SLOTS)],
            device_id={"row": 1 - my_row},
            device_id_type=MESH,
        )

    def begin(u):
        return jnp.where((my_row == 0) & (u < early), 1, 0) if zone else 0

    def swap_factors():
        for j in range(1, groups):
            pass_factors(j).wait_send()
            part = tbuf.at[pl.ds(lax.rem(my_row + groups - j, groups) * share, share)]
            pltpu.make_async_remote_copy(
                src_ref=part,
                dst_ref=part,
                send_sem=tsnd.at[j - 1],
                recv_sem=trcv.at[j - 1],
                device_id={"row": lax.rem(my_row + j, groups)},
                device_id_type=MESH,
            ).wait_recv()

    def partial(sl, j):
        return pltpu.make_async_remote_copy(
            src_ref=psend.at[sl],
            dst_ref=precv.at[sl, j - 1],
            send_sem=psnd.at[sl, j - 1],
            recv_sem=prcv.at[sl, j - 1],
            device_id={"row": lax.rem(my_row + j, groups)},
            device_id_type=MESH,
        )

    def project(u):
        spot, h = lax.rem(u // H, ring), lax.rem(u, H)
        sl = lax.rem(u, 2 * H)
        if zone:

            @pl.when((my_row == 1) & (u < early))
            def _():
                hand(u).wait_recv()

        part = pl.ds(0, members * sub)
        acc[part] = jnp.zeros((members * sub, acc.shape[1]), jnp.float32)

        def body(n, _):
            at = pl.multiple_of(n * tile, tile)
            left = halves(vbuf[spot, h, :, :, pl.ds(at, tile)].reshape(members * sub, tile))
            right = halves(zbuf[pl.ds(at, tile), :])
            acc[part] += dot3(left, right, 1, 0)
            return 0

        lax.fori_loop(begin(u), rows // tile, body, 0)
        psend[sl] = acc[part]
        for j in range(1, groups):
            partial(sl, j).start()

    def store(n):
        spot = pl.ds(pl.multiple_of(n * tile, tile), tile)
        return pltpu.make_async_copy(zbuf.at[spot], out_ref.at[spot], zsem)

    def update(i, last):
        base = lax.rem(i, 2) * H
        total = []
        for h in range(H):
            whole_sum = psend[base + h]
            for j in range(1, groups):
                partial(base + h, j).wait()
                whole_sum = whole_sum + precv[base + h, j - 1]
            total.append(whole_sum)
        total = halves(jnp.concatenate(total, axis=0))
        spot = lax.rem(i, ring)
        factor = halves(tbuf[panels - 1 - i].reshape(width, width))
        scaled = dot3(factor, total, 0, 0)
        for h in range(H):
            for owner in range(members):
                at = (owner * H + h) * sub
                acc[pl.ds((h * members + owner) * sub, sub), :] = scaled[at : at + sub]
        scaled = halves(acc[...])

        def body(n, _):
            at = pl.multiple_of(n * tile, tile)
            left = halves(vbuf[spot, :, :, :, pl.ds(at, tile)].reshape(width, tile))
            zbuf[pl.ds(at, tile), :] = zbuf[pl.ds(at, tile), :] - dot3(left, scaled, 0, 0)
            if last:

                @pl.when(n > 0)
                def _():
                    store(n - 1).start()

            return 0

        lax.fori_loop(0 if last else begin(i * H), rows // tile, body, 0)

    barrier = pltpu.get_barrier_semaphore()

    def greet(target):
        pl.semaphore_signal(barrier, inc=1, device_id=target, device_id_type=MESH)

    pl.when(a < A - 1)(lambda: greet({"col": index(a + 1, b, c)}))
    pl.when(a > 0)(lambda: greet({"col": index(a - 1, b, c)}))
    for j in range(1, B):
        greet({"col": index(a, lax.rem(b + j, B), c)})
    greet({"col": index(a, b, 1 - c)})
    for j in range(1, groups):
        greet({"row": lax.rem(my_row + j, groups)})
    beyond = jnp.where(a < A - 1, 1, 0) + jnp.where(a > 0, 1, 0)
    pl.semaphore_wait(barrier, beyond + (B + groups - 1))

    fetch = pltpu.make_async_copy(z_hbm, zbuf, zsem)
    if zone:

        @pl.when(my_row == 1)
        def _():
            lend().start()

    for u in range(AHEAD):
        hop(jnp.int32(u), 0, True, (0,))
    fetch.start()
    own_factors().start()
    if zone:

        @pl.when(my_row == 0)
        def _():
            lend().wait_recv()

    for u in range(AHEAD):
        hop(jnp.int32(u), 0, True, (1,))
    fetch.wait()

    def slot(t, _):
        w = t - A

        @pl.when(w >= 0)
        def _():
            i, h = w // H, lax.rem(w, H)

            @pl.when((h == 0) & (i == 1))
            def _():
                swap_factors()

            @pl.when((h == 0) & (w > 0))
            def _():
                update(i - 1, False)

            project(w)

        for h in range(A, 0, -1):
            u = t - (h - 1)

            @pl.when((u >= 0) & (u < units))
            def _(u=u, h=h):
                hop(u, h, True)

        @pl.when(t + AHEAD < units)
        def _():
            hop(t + AHEAD, 0, True)

        v = t - A + 1

        @pl.when((v >= 0) & (v < units))
        def _():
            settle(v)

        @pl.when(w >= 0)
        def _():
            for h in range(A + 1):
                hop(w, h, False)
            if zone:

                @pl.when((my_row == 0) & (w < early))
                def _():
                    hand(w).wait_send()

        return 0

    lax.fori_loop(0, units + A, slot, 0)
    update(jnp.int32(panels - 1), True)
    if zone:

        @pl.when(my_row == 1)
        def _():
            lend().wait_send()

    store(rows // tile - 1).start()
    pltpu.make_async_copy(zbuf, out_ref, zsem).wait()


def local(eigvecs, v_panels, t_panels):
    panels, rows, per = v_panels.shape
    width = t_panels.shape[1]
    groups = lax.axis_size("row")
    members = lax.axis_size("col")
    chips = members // 2
    B = max(n for n in range(1, chips + 1) if chips % n == 0 and n * n <= chips)
    A = chips // B
    columns = eigvecs.shape[1]
    H = per // 8 if per % 8 == 0 else 1
    sub = per // H
    vectors = jnp.transpose(v_panels, (0, 2, 1)).reshape(panels, H, sub, rows)
    factors = jnp.transpose(t_panels, (0, 2, 1)).reshape(panels, H, sub, width)
    dma = pltpu.SemaphoreType.DMA
    anywhere = pl.BlockSpec(memory_space=pl.ANY)
    others = max(groups - 1, 1)
    ring = min(panels, 1 + (A + AHEAD + 2 + H - 1) // H)
    tile = min(rows, 1024)
    zone = tile if groups == 2 and rows >= 4 * tile and tile % (2 * width) == 0 and tile < panels * width else 0
    lent = (panels - zone // width, H, sub, zone // 2) if zone else (1, H, sub, 128)
    out = pl.pallas_call(
        functools.partial(kernel, (groups, A, B, zone, tile)),
        out_shape=jax.ShapeDtypeStruct((rows, columns), jnp.float32),
        in_specs=[anywhere] * 3,
        out_specs=anywhere,
        scratch_shapes=[
            pltpu.VMEM((rows, columns), jnp.float32),
            pltpu.VMEM((ring, H, members, sub, rows), jnp.float32),
            pltpu.VMEM((panels, H, members, sub, width), jnp.float32),
            pltpu.VMEM(lent, jnp.float32),
            pltpu.VMEM((width, columns), jnp.float32),
            pltpu.VMEM((2 * H, members * sub, columns), jnp.float32),
            pltpu.VMEM((2 * H, others, members * sub, columns), jnp.float32),
            dma((SLOTS, 3, members)),
            dma((SLOTS, 3, chips)),
            dma((SLOTS, 3, chips)),
            dma((SLOTS, 2 * A + 1, max(B - 1, 1))),
            dma((SLOTS, 3, chips)),
            dma((SLOTS,)),
            dma,
            dma((2 * H, others)),
            dma((2 * H, others)),
            dma,
            dma((others,)),
            dma((others,)),
            dma,
            dma,
            dma((SLOTS,)),
            dma((SLOTS,)),
        ],
        compiler_params=pltpu.CompilerParams(
            collective_id=0, has_side_effects=True, vmem_limit_bytes=54 * 2**20
        ),
    )(eigvecs, vectors, factors)
    return out


def solution(mesh):
    in_specs = (P("row", "col"), P(None, "row", "col"), P(None, None, "col"))
    out_specs = P("row", "col")
    return jax.shard_map(local, mesh=mesh, in_specs=in_specs, out_specs=out_specs, check_vma=False)
```

```python
import functools

import jax
import jax.numpy as jnp
from jax import lax
from jax.experimental import pallas as pl
from jax.experimental.pallas import tpu as pltpu
from jax.sharding import PartitionSpec as P

SLOTS = 8
SENDS = 4
AHEAD = 2
MESH = pl.DeviceIdType.MESH


def halves(x):
    high = x.astype(jnp.bfloat16)
    return high, (x - high.astype(jnp.float32)).astype(jnp.bfloat16)


def dot3(left, right, left_axis, right_axis):
    def one(a, b):
        return lax.dot_general(
            a, b, (((left_axis,), (right_axis,)), ((), ())), preferred_element_type=jnp.float32
        )

    (lh, ll), (rh, rl) = left, right
    return one(lh, rh) + (one(ll, rh) + one(lh, rl))


def kernel(shape, z_hbm, v_ref, t_ref, out_ref, zbuf, vbuf, tbuf, stage, acc, psend, precv, *sems):
    groups, A, B, zone, tile = shape
    recv, rside, rpair, su, sd, sy, sc, tu, td, ty, tc, tr = sems[:12]
    lsem, zsem, psnd, prcv, town, tsnd, trcv, lsnd, lrcv, gsnd, grcv = sems[12:]
    panels, H, sub, rows = v_ref.shape
    members = 2 * A * B
    ring = vbuf.shape[0]
    width = H * members * sub
    units = panels * H
    share = panels // groups
    tiles = rows // 128
    spare = (B - 1) * A - (A - 1)
    whole = 2 * max((A - 1) * (B - 1), 1)
    side = min(max((tiles * spare + whole // 2) // whole, 1), tiles - 1)
    cut = (tiles - side) * 128
    half = zone // 2
    floor = zone // width
    early = (panels - floor) * H if zone else 0
    me = lax.axis_index("col")
    my_row = lax.axis_index("row")
    c = lax.rem(me, 2)
    b = lax.rem(me // 2, B)
    a = me // (2 * B)
    mine = pl.ds(my_row * share, share)

    def index(aa, bb, cc):
        return (aa * B + bb) * 2 + cc

    def place(u, owner, lo, hi):
        return vbuf.at[lax.rem(u // H, ring), lax.rem(u, H), owner, :, pl.ds(lo, hi - lo)]

    def sized(u, body):
        if zone:
            pl.when(u < early)(lambda: body(half))
            pl.when(u >= early)(lambda: body(0))
        else:
            body(0)

    def landed(spot, sem):
        pltpu.make_async_remote_copy(
            src_ref=spot,
            dst_ref=spot,
            send_sem=sc.at[0, 0],
            recv_sem=sem,
            device_id={"col": index(a, b, 1 - c)},
            device_id_type=MESH,
        ).wait_recv()

    def source(u, span):
        return v_ref.at[panels - 1 - u // H, lax.rem(u, H), :, span]

    def slot_of(u, span):
        return vbuf.at[lax.rem(u // H, ring), lax.rem(u, H), me, :, span]

    def staged(u):
        return stage.at[panels - 1 - u // H - floor, lax.rem(u, H)]

    low, mid, high = pl.ds(0, half), pl.ds(half, zone - half), pl.ds(zone, rows - zone)

    def lent(u, body):
        borrowed = (my_row == 0) & (u < early)
        pl.when(borrowed)(lambda: body(staged(u)))

    def hop(u, h, go, stages=(0, 1)):
        sl = lax.rem(u, SLOTS)
        ts = lax.rem(u + (h - 1 if h else SENDS - AHEAD), SENDS)

        def copy(src, dst, target, send_sem, recv_sem):
            return pltpu.make_async_remote_copy(
                src_ref=src,
                dst_ref=dst,
                send_sem=send_sem,
                recv_sem=recv_sem,
                device_id={"col": target},
                device_id_type=MESH,
            )

        def move(owner, stop, target, send_sem, recv_sem):
            def part(src, lo, hi):
                copy(src, place(u, owner, lo, hi), target, send_sem, recv_sem).start()

            def fresh(lo, hi):
                part(source(u, pl.ds(lo, hi - lo)), lo, hi)

            def passed(lo, hi):
                spot = place(u, owner, lo, hi)
                one = copy(spot, spot, target, send_sem, recv_sem)
                one.start() if go else one.wait_send()

            if not go or h:
                if stop is None:
                    passed(cut, rows)
                else:
                    sized(u, lambda start: passed(start, stop))
            elif stop is None:
                if 0 in stages:
                    fresh(cut, rows)
            elif zone:
                borrowed = (my_row == 0) & (u < early)
                if 0 in stages:
                    pl.when(borrowed)(lambda: fresh(zone, stop))
                    pl.when(jnp.logical_not(borrowed) & (u < early))(lambda: fresh(half, stop))
                    pl.when(u >= early)(lambda: fresh(0, stop))
                if 1 in stages:
                    pl.when(borrowed)(lambda: part(staged(u), half, zone))
            elif 0 in stages:
                fresh(0, stop)

        def move_factor(owner, target, send_sem, recv_sem):
            spot = tbuf.at[mine, :, owner]
            one = copy(spot if h else t_ref.at[mine], spot, target, send_sem, recv_sem)
            one.start() if go else one.wait_send()

        def both(sg, body):
            if sg >= 0:
                pl.when(a < A - 1)(lambda: body(index(a + 1, b, c), 0))
            if sg <= 0:
                pl.when(a > 0)(lambda: body(index(a - 1, b, c), 1))

        def signs(d):
            return (1, -1) if d else (0,)

        def facing(d, body):
            if d < A:
                for sg in signs(d):
                    at = a - sg * d
                    if d == 0:
                        body(sg, at)
                    else:
                        pl.when((at >= 0) & (at < A))(functools.partial(body, sg, at))

        def forward(sg, at):
            owner, cid = index(at, b, c), at * B + b
            both(sg, lambda to, way: move(owner, rows, to, (su, sd)[way].at[ts, at * B], recv.at[sl, cid]))
            for j in range(1, B):
                to = index(a, lax.rem(b + j, B), c)
                if h == 0:
                    side = at * (B - 1) + (B - j - 1)
                    move(owner, None, to, sy.at[ts, A, j - 1], rside.at[sl, side])
                move(owner, cut, to, sy.at[ts, at, j - 1], recv.at[sl, cid])
            move(owner, rows, index(a, b, 1 - c), sc.at[ts, cid], rpair.at[sl, cid])

            if 0 in stages:

                @pl.when(u == 0)
                def _():
                    both(sg, lambda to, way: move_factor(owner, to, (tu, td)[way].at[at], tr.at[0, cid]))
                    for j in range(1, B):
                        to = index(a, lax.rem(b + j, B), c)
                        move_factor(owner, to, ty.at[at, j - 1], tr.at[0, cid])
                    move_factor(owner, index(a, b, 1 - c), tc.at[cid], tr.at[1, cid])

        def straight(sg, at):
            owner, cid = index(at, b, c), at * B + b
            if go:
                sized(u, lambda start: landed(place(u, owner, start, rows), recv.at[sl, cid]))
                pl.when(u == 0)(lambda: landed(tbuf.at[mine, :, owner], tr.at[0, cid]))
            forward(sg, at)

        def turned(sg, at):
            for j in range(1, B):
                owner, side = index(at, lax.rem(b + j, B), c), at * (B - 1) + (j - 1)
                if go:
                    landed(place(u, owner, cut, rows), rside.at[sl, side])
                both(sg, lambda to, way: move(owner, None, to, (su, sd)[way].at[ts, at * B + j], rside.at[sl, side]))

        def crossed(sg, at):
            for j in range(1, B):
                bb = lax.rem(b + j, B)
                owner, cid = index(at, bb, c), at * B + bb
                if go:
                    sized(u, lambda start: landed(place(u, owner, start, cut), recv.at[sl, cid]))
                    pl.when(u == 0)(lambda: landed(tbuf.at[mine, :, owner], tr.at[0, cid]))
                move(owner, rows, index(a, b, 1 - c), sc.at[ts, cid], rpair.at[sl, cid])

                @pl.when(u == 0)
                def _():
                    move_factor(owner, index(a, b, 1 - c), tc.at[cid], tr.at[1, cid])

        if h == 0:
            forward(0, a)
            if 1 in stages and go:
                own_vectors(u)
            return

        facing(h, straight)
        facing(h - 1, turned)
        facing(h - 1, crossed)

    def pass_factors(j):
        return pltpu.make_async_remote_copy(
            src_ref=tbuf.at[mine],
            dst_ref=tbuf.at[mine],
            send_sem=tsnd.at[j - 1],
            recv_sem=trcv.at[j - 1],
            device_id={"row": lax.rem(my_row + j, groups)},
            device_id_type=MESH,
        )

    def own_factors():
        return pltpu.make_async_copy(t_ref.at[mine], tbuf.at[mine, :, me], town)

    def settle(u):
        for at in range(A):
            for bb in range(B):
                owner, sem = index(at, bb, 1 - c), rpair.at[lax.rem(u, SLOTS), at * B + bb]
                sized(u, lambda start: landed(place(u, owner, start, rows), sem))

        if zone:

            @pl.when(u >= early)
            def _():
                own_arrived(u, pl.ds(0, rows))

            @pl.when(u < early)
            def _():
                own_arrived(u, pl.ds(half, rows - half))

                @pl.when(my_row == 0)
                def _():
                    hand(u).start()
        else:
            own_arrived(u, pl.ds(0, rows))

        @pl.when(u == 0)
        def _():
            for at in range(A):
                for bb in range(B):
                    landed(tbuf.at[mine, :, index(at, bb, 1 - c)], tr.at[1, at * B + bb])
            own_factors().wait()
            for j in range(1, groups):
                pass_factors(j).start()

    def own_vectors(u):
        def fetch_own(src, span):
            pltpu.make_async_copy(src, slot_of(u, span), lsem.at[lax.rem(u, SLOTS)]).start()

        if zone:
            lent(u, lambda src: fetch_own(src, mid))
            rest = pl.ds(half, rows - half)
            borrowed = (my_row == 0) & (u < early)
            pl.when(borrowed)(lambda: fetch_own(source(u, high), high))
            pl.when(jnp.logical_not(borrowed) & (u < early))(lambda: fetch_own(source(u, rest), rest))
            pl.when(u >= early)(lambda: fetch_own(source(u, pl.ds(0, rows)), pl.ds(0, rows)))
        else:
            fetch_own(source(u, pl.ds(0, rows)), pl.ds(0, rows))

    def own_arrived(u, span):
        pltpu.make_async_copy(source(u, span), slot_of(u, span), lsem.at[lax.rem(u, SLOTS)]).wait()

    def lend():
        return pltpu.make_async_remote_copy(
            src_ref=v_ref.at[pl.ds(floor, panels - floor), :, :, low],
            dst_ref=stage,
            send_sem=lsnd,
            recv_sem=lrcv,
            device_id={"row": 1 - my_row},
            device_id_type=MESH,
        )

    def hand(u):
        spot, h = lax.rem(u // H, ring), lax.rem(u, H)
        return pltpu.make_async_remote_copy(
            src_ref=vbuf.at[spot, h, :, :, mid],
            dst_ref=vbuf.at[spot, h, :, :, low],
            send_sem=gsnd.at[lax.rem(u, SLOTS)],
            recv_sem=grcv.at[lax.rem(u, SLOTS)],
            device_id={"row": 1 - my_row},
            device_id_type=MESH,
        )

    def begin(u):
        return jnp.where((my_row == 0) & (u < early), 1, 0) if zone else 0

    def swap_factors():
        for j in range(1, groups):
            pass_factors(j).wait_send()
            part = tbuf.at[pl.ds(lax.rem(my_row + groups - j, groups) * share, share)]
            pltpu.make_async_remote_copy(
                src_ref=part,
                dst_ref=part,
                send_sem=tsnd.at[j - 1],
                recv_sem=trcv.at[j - 1],
                device_id={"row": lax.rem(my_row + j, groups)},
                device_id_type=MESH,
            ).wait_recv()

    def partial(sl, j):
        return pltpu.make_async_remote_copy(
            src_ref=psend.at[sl],
            dst_ref=precv.at[sl, j - 1],
            send_sem=psnd.at[sl, j - 1],
            recv_sem=prcv.at[sl, j - 1],
            device_id={"row": lax.rem(my_row + j, groups)},
            device_id_type=MESH,
        )

    def project(u):
        spot, h = lax.rem(u // H, ring), lax.rem(u, H)
        sl = lax.rem(u, 2 * H)
        if zone:

            @pl.when((my_row == 1) & (u < early))
            def _():
                hand(u).wait_recv()

        part = pl.ds(0, members * sub)
        acc[part] = jnp.zeros((members * sub, acc.shape[1]), jnp.float32)

        def body(n, _):
            at = pl.multiple_of(n * tile, tile)
            left = halves(vbuf[spot, h, :, :, pl.ds(at, tile)].reshape(members * sub, tile))
            right = halves(zbuf[pl.ds(at, tile), :])
            acc[part] += dot3(left, right, 1, 0)
            return 0

        lax.fori_loop(begin(u), rows // tile, body, 0)
        psend[sl] = acc[part]
        for j in range(1, groups):
            partial(sl, j).start()

    def store(n):
        spot = pl.ds(pl.multiple_of(n * tile, tile), tile)
        return pltpu.make_async_copy(zbuf.at[spot], out_ref.at[spot], zsem)

    def update(i, last):
        base = lax.rem(i, 2) * H
        total = []
        for h in range(H):
            whole_sum = psend[base + h]
            for j in range(1, groups):
                partial(base + h, j).wait()
                whole_sum = whole_sum + precv[base + h, j - 1]
            total.append(whole_sum)
        total = halves(jnp.concatenate(total, axis=0))
        spot = lax.rem(i, ring)
        factor = halves(tbuf[panels - 1 - i].reshape(width, width))
        scaled = dot3(factor, total, 0, 0)
        for h in range(H):
            for owner in range(members):
                at = (owner * H + h) * sub
                acc[pl.ds((h * members + owner) * sub, sub), :] = scaled[at : at + sub]
        scaled = halves(acc[...])

        def body(n, _):
            at = pl.multiple_of(n * tile, tile)
            left = halves(vbuf[spot, :, :, :, pl.ds(at, tile)].reshape(width, tile))
            zbuf[pl.ds(at, tile), :] = zbuf[pl.ds(at, tile), :] - dot3(left, scaled, 0, 0)
            if last:

                @pl.when(n > 0)
                def _():
                    store(n - 1).start()

            return 0

        lax.fori_loop(0 if last else begin(i * H), rows // tile, body, 0)

    barrier = pltpu.get_barrier_semaphore()

    def greet(target):
        pl.semaphore_signal(barrier, inc=1, device_id=target, device_id_type=MESH)

    pl.when(a < A - 1)(lambda: greet({"col": index(a + 1, b, c)}))
    pl.when(a > 0)(lambda: greet({"col": index(a - 1, b, c)}))
    for j in range(1, B):
        greet({"col": index(a, lax.rem(b + j, B), c)})
    greet({"col": index(a, b, 1 - c)})
    for j in range(1, groups):
        greet({"row": lax.rem(my_row + j, groups)})
    beyond = jnp.where(a < A - 1, 1, 0) + jnp.where(a > 0, 1, 0)
    pl.semaphore_wait(barrier, beyond + (B + groups - 1))

    fetch = pltpu.make_async_copy(z_hbm, zbuf, zsem)
    if zone:

        @pl.when(my_row == 1)
        def _():
            lend().start()

    for u in range(AHEAD):
        hop(jnp.int32(u), 0, True, (0,))
    fetch.start()
    own_factors().start()
    if zone:

        @pl.when(my_row == 0)
        def _():
            lend().wait_recv()

    for u in range(AHEAD):
        hop(jnp.int32(u), 0, True, (1,))
    fetch.wait()

    def slot(t, _):
        w = t - A

        @pl.when((w >= 0) & (w < units))
        def _():
            i, h = w // H, lax.rem(w, H)

            @pl.when((h == 0) & (i == 1))
            def _():
                swap_factors()

            @pl.when((h == 0) & (w > 0))
            def _():
                update(i - 1, False)

            project(w)

        for h in range(A, 0, -1):
            u = t - (h - 1)

            @pl.when((u >= 0) & (u < units))
            def _(u=u, h=h):
                hop(u, h, True)

        @pl.when(t + AHEAD < units)
        def _():
            hop(t + AHEAD, 0, True)

        v = t - A + 1

        @pl.when((v >= 0) & (v < units))
        def _():
            settle(v)

        for h in range(A + 1):
            u = t - (SENDS - 1) - (h - 1 if h else -AHEAD)

            @pl.when((u >= 0) & (u < units))
            def _(u=u, h=h):
                hop(u, h, False)

        if zone:

            @pl.when((my_row == 0) & (w >= 0) & (w < early))
            def _():
                hand(w).wait_send()

        return 0

    lax.fori_loop(0, units + A + SENDS - 2, slot, 0)
    update(jnp.int32(panels - 1), True)
    if zone:

        @pl.when(my_row == 1)
        def _():
            lend().wait_send()

    store(rows // tile - 1).start()
    pltpu.make_async_copy(zbuf, out_ref, zsem).wait()


def local(eigvecs, v_panels, t_panels):
    panels, rows, per = v_panels.shape
    width = t_panels.shape[1]
    groups = lax.axis_size("row")
    members = lax.axis_size("col")
    chips = members // 2
    B = max(n for n in range(1, chips + 1) if chips % n == 0 and n * n <= chips)
    A = chips // B
    columns = eigvecs.shape[1]
    H = per // 8 if per % 8 == 0 else 1
    sub = per // H
    vectors = jnp.transpose(v_panels, (0, 2, 1)).reshape(panels, H, sub, rows)
    factors = jnp.transpose(t_panels, (0, 2, 1)).reshape(panels, H, sub, width)
    dma = pltpu.SemaphoreType.DMA
    anywhere = pl.BlockSpec(memory_space=pl.ANY)
    others = max(groups - 1, 1)
    ring = min(panels, 1 + (A + AHEAD + 2 + H - 1) // H)
    tile = min(rows, 1024)
    zone = tile if groups == 2 and rows >= 4 * tile and tile % (2 * width) == 0 and tile < panels * width else 0
    lent = (panels - zone // width, H, sub, zone // 2) if zone else (1, H, sub, 128)
    out = pl.pallas_call(
        functools.partial(kernel, (groups, A, B, zone, tile)),
        out_shape=jax.ShapeDtypeStruct((rows, columns), jnp.float32),
        in_specs=[anywhere] * 3,
        out_specs=anywhere,
        scratch_shapes=[
            pltpu.VMEM((rows, columns), jnp.float32),
            pltpu.VMEM((ring, H, members, sub, rows), jnp.float32),
            pltpu.VMEM((panels, H, members, sub, width), jnp.float32),
            pltpu.VMEM(lent, jnp.float32),
            pltpu.VMEM((width, columns), jnp.float32),
            pltpu.VMEM((2 * H, members * sub, columns), jnp.float32),
            pltpu.VMEM((2 * H, others, members * sub, columns), jnp.float32),
            dma((SLOTS, chips)),
            dma((SLOTS, A * max(B - 1, 1))),
            dma((SLOTS, chips)),
            dma((SENDS, chips)),
            dma((SENDS, chips)),
            dma((SENDS, A + 1, max(B - 1, 1))),
            dma((SENDS, chips)),
            dma((A,)),
            dma((A,)),
            dma((A, max(B - 1, 1))),
            dma((chips,)),
            dma((2, chips)),
            dma((SLOTS,)),
            dma,
            dma((2 * H, others)),
            dma((2 * H, others)),
            dma,
            dma((others,)),
            dma((others,)),
            dma,
            dma,
            dma((SLOTS,)),
            dma((SLOTS,)),
        ],
        compiler_params=pltpu.CompilerParams(
            collective_id=0, has_side_effects=True, vmem_limit_bytes=54 * 2**20
        ),
    )(eigvecs, vectors, factors)
    return out


def solution(mesh):
    in_specs = (P("row", "col"), P(None, "row", "col"), P(None, None, "col"))
    out_specs = P("row", "col")
    return jax.shard_map(local, mesh=mesh, in_specs=in_specs, out_specs=out_specs, check_vma=False)
```

```python
import functools

import jax
import jax.numpy as jnp
from jax import lax
from jax.experimental import pallas as pl
from jax.experimental.pallas import tpu as pltpu
from jax.sharding import PartitionSpec as P

SLOTS = 8
SENDS = 4
AHEAD = 2
MESH = pl.DeviceIdType.MESH


def halves(x):
    high = x.astype(jnp.bfloat16)
    return high, (x - high.astype(jnp.float32)).astype(jnp.bfloat16)


def dot3(left, right, left_axis, right_axis):
    def one(a, b):
        return lax.dot_general(
            a, b, (((left_axis,), (right_axis,)), ((), ())), preferred_element_type=jnp.float32
        )

    (lh, ll), (rh, rl) = left, right
    return one(lh, rh) + (one(ll, rh) + one(lh, rl))


def kernel(shape, z_hbm, v_ref, t_ref, out_ref, zbuf, vbuf, tbuf, stage, acc, psend, precv, *sems):
    groups, A, B, zone, tile = shape
    recv, rside, rpair, su, sd, sy, sc, tu, td, ty, tc, tr = sems[:12]
    lsem, zsem, psnd, prcv, town, tsnd, trcv, lsnd, lrcv, gsnd, grcv = sems[12:]
    panels, H, sub, rows = v_ref.shape
    members = 2 * A * B
    ring = vbuf.shape[0]
    width = H * members * sub
    units = panels * H
    share = panels // groups
    tiles = rows // 128
    spare = (B - 1) * A - (A - 1)
    whole = 2 * max((A - 1) * (B - 1), 1)
    side = min(max((tiles * spare + whole // 2) // whole, 1), tiles - 1)
    cut = (tiles - side) * 128
    half = zone // 2

    def is_early(u):
        return (u > 0) & (u < early)

    floor = zone // width
    early = (panels - floor) * H if zone else 0
    me = lax.axis_index("col")
    my_row = lax.axis_index("row")
    c = lax.rem(me, 2)
    b = lax.rem(me // 2, B)
    a = me // (2 * B)
    mine = pl.ds(my_row * share, share)

    def index(aa, bb, cc):
        return (aa * B + bb) * 2 + cc

    def place(u, owner, lo, hi):
        return vbuf.at[lax.rem(u // H, ring), lax.rem(u, H), owner, :, pl.ds(lo, hi - lo)]

    def sized(u, body):
        if zone:
            pl.when(is_early(u))(lambda: body(half))
            pl.when(jnp.logical_not(is_early(u)))(lambda: body(0))
        else:
            body(0)

    def landed(spot, sem):
        pltpu.make_async_remote_copy(
            src_ref=spot,
            dst_ref=spot,
            send_sem=sc.at[0, 0],
            recv_sem=sem,
            device_id={"col": index(a, b, 1 - c)},
            device_id_type=MESH,
        ).wait_recv()

    def source(u, span):
        return v_ref.at[panels - 1 - u // H, lax.rem(u, H), :, span]

    def slot_of(u, span):
        return vbuf.at[lax.rem(u // H, ring), lax.rem(u, H), me, :, span]

    def staged(u):
        return stage.at[panels - 1 - u // H - floor, lax.rem(u, H)]

    low, mid, high = pl.ds(0, half), pl.ds(half, zone - half), pl.ds(zone, rows - zone)

    def lent(u, body):
        borrowed = (my_row == 0) & (is_early(u))
        pl.when(borrowed)(lambda: body(staged(u)))

    def hop(u, h, go, stages=(0, 1)):
        sl = lax.rem(u, SLOTS)
        ts = lax.rem(u + (h - 1 if h else SENDS - AHEAD), SENDS)

        def copy(src, dst, target, send_sem, recv_sem):
            return pltpu.make_async_remote_copy(
                src_ref=src,
                dst_ref=dst,
                send_sem=send_sem,
                recv_sem=recv_sem,
                device_id={"col": target},
                device_id_type=MESH,
            )

        def move(owner, stop, target, send_sem, recv_sem):
            def part(src, lo, hi):
                copy(src, place(u, owner, lo, hi), target, send_sem, recv_sem).start()

            def fresh(lo, hi):
                part(source(u, pl.ds(lo, hi - lo)), lo, hi)

            def passed(lo, hi):
                spot = place(u, owner, lo, hi)
                one = copy(spot, spot, target, send_sem, recv_sem)
                one.start() if go else one.wait_send()

            if not go or h:
                if stop is None:
                    passed(cut, rows)
                else:
                    sized(u, lambda start: passed(start, stop))
            elif stop is None:
                if 0 in stages:
                    fresh(cut, rows)
            elif zone:
                borrowed = (my_row == 0) & (is_early(u))
                if 0 in stages:
                    pl.when(borrowed)(lambda: fresh(zone, stop))
                    pl.when(jnp.logical_not(borrowed) & (is_early(u)))(lambda: fresh(half, stop))
                    pl.when(jnp.logical_not(is_early(u)))(lambda: fresh(0, stop))
                if 1 in stages:
                    pl.when(borrowed)(lambda: part(staged(u), half, zone))
            elif 0 in stages:
                fresh(0, stop)

        def move_factor(owner, target, send_sem, recv_sem):
            spot = tbuf.at[mine, :, owner]
            one = copy(spot if h else t_ref.at[mine], spot, target, send_sem, recv_sem)
            one.start() if go else one.wait_send()

        def both(sg, body):
            if sg >= 0:
                pl.when(a < A - 1)(lambda: body(index(a + 1, b, c), 0))
            if sg <= 0:
                pl.when(a > 0)(lambda: body(index(a - 1, b, c), 1))

        def signs(d):
            return (1, -1) if d else (0,)

        def facing(d, body):
            if d < A:
                for sg in signs(d):
                    at = a - sg * d
                    if d == 0:
                        body(sg, at)
                    else:
                        pl.when((at >= 0) & (at < A))(functools.partial(body, sg, at))

        def forward(sg, at):
            owner, cid = index(at, b, c), at * B + b
            both(sg, lambda to, way: move(owner, rows, to, (su, sd)[way].at[ts, at * B], recv.at[sl, cid]))
            for j in range(1, B):
                to = index(a, lax.rem(b + j, B), c)
                if h == 0:
                    side = at * (B - 1) + (B - j - 1)
                    move(owner, None, to, sy.at[ts, A, j - 1], rside.at[sl, side])
                move(owner, cut, to, sy.at[ts, at, j - 1], recv.at[sl, cid])
            move(owner, rows, index(a, b, 1 - c), sc.at[ts, cid], rpair.at[sl, cid])

            if 0 in stages:

                @pl.when(u == 0)
                def _():
                    both(sg, lambda to, way: move_factor(owner, to, (tu, td)[way].at[at], tr.at[0, cid]))
                    for j in range(1, B):
                        to = index(a, lax.rem(b + j, B), c)
                        move_factor(owner, to, ty.at[at, j - 1], tr.at[0, cid])
                    move_factor(owner, index(a, b, 1 - c), tc.at[cid], tr.at[1, cid])

        def straight(sg, at):
            owner, cid = index(at, b, c), at * B + b
            if go:
                sized(u, lambda start: landed(place(u, owner, start, rows), recv.at[sl, cid]))
                pl.when(u == 0)(lambda: landed(tbuf.at[mine, :, owner], tr.at[0, cid]))
            forward(sg, at)

        def turned(sg, at):
            for j in range(1, B):
                owner, side = index(at, lax.rem(b + j, B), c), at * (B - 1) + (j - 1)
                if go:
                    landed(place(u, owner, cut, rows), rside.at[sl, side])
                both(sg, lambda to, way: move(owner, None, to, (su, sd)[way].at[ts, at * B + j], rside.at[sl, side]))

        def crossed(sg, at):
            for j in range(1, B):
                bb = lax.rem(b + j, B)
                owner, cid = index(at, bb, c), at * B + bb
                if go:
                    sized(u, lambda start: landed(place(u, owner, start, cut), recv.at[sl, cid]))
                    pl.when(u == 0)(lambda: landed(tbuf.at[mine, :, owner], tr.at[0, cid]))
                move(owner, rows, index(a, b, 1 - c), sc.at[ts, cid], rpair.at[sl, cid])

                @pl.when(u == 0)
                def _():
                    move_factor(owner, index(a, b, 1 - c), tc.at[cid], tr.at[1, cid])

        if h == 0:
            forward(0, a)
            if 1 in stages and go:
                own_vectors(u)
            return

        facing(h, straight)
        facing(h - 1, turned)
        facing(h - 1, crossed)

    def pass_factors(j):
        return pltpu.make_async_remote_copy(
            src_ref=tbuf.at[mine],
            dst_ref=tbuf.at[mine],
            send_sem=tsnd.at[j - 1],
            recv_sem=trcv.at[j - 1],
            device_id={"row": lax.rem(my_row + j, groups)},
            device_id_type=MESH,
        )

    def own_factors():
        return pltpu.make_async_copy(t_ref.at[mine], tbuf.at[mine, :, me], town)

    def settle(u):
        for at in range(A):
            for bb in range(B):
                owner, sem = index(at, bb, 1 - c), rpair.at[lax.rem(u, SLOTS), at * B + bb]
                sized(u, lambda start: landed(place(u, owner, start, rows), sem))

        if zone:

            @pl.when(jnp.logical_not(is_early(u)))
            def _():
                own_arrived(u, pl.ds(0, rows))

            @pl.when(is_early(u))
            def _():
                own_arrived(u, pl.ds(half, rows - half))

                @pl.when(my_row == 0)
                def _():
                    hand(u).start()
        else:
            own_arrived(u, pl.ds(0, rows))

        @pl.when(u == 0)
        def _():
            for at in range(A):
                for bb in range(B):
                    landed(tbuf.at[mine, :, index(at, bb, 1 - c)], tr.at[1, at * B + bb])
            own_factors().wait()
            for j in range(1, groups):
                pass_factors(j).start()

    def own_vectors(u):
        def fetch_own(src, span):
            pltpu.make_async_copy(src, slot_of(u, span), lsem.at[lax.rem(u, SLOTS)]).start()

        if zone:
            lent(u, lambda src: fetch_own(src, mid))
            rest = pl.ds(half, rows - half)
            borrowed = (my_row == 0) & (is_early(u))
            pl.when(borrowed)(lambda: fetch_own(source(u, high), high))
            pl.when(jnp.logical_not(borrowed) & (is_early(u)))(lambda: fetch_own(source(u, rest), rest))
            pl.when(jnp.logical_not(is_early(u)))(lambda: fetch_own(source(u, pl.ds(0, rows)), pl.ds(0, rows)))
        else:
            fetch_own(source(u, pl.ds(0, rows)), pl.ds(0, rows))

    def own_arrived(u, span):
        pltpu.make_async_copy(source(u, span), slot_of(u, span), lsem.at[lax.rem(u, SLOTS)]).wait()

    def lend():
        return pltpu.make_async_remote_copy(
            src_ref=v_ref.at[pl.ds(floor, panels - floor), :, :, low],
            dst_ref=stage,
            send_sem=lsnd,
            recv_sem=lrcv,
            device_id={"row": 1 - my_row},
            device_id_type=MESH,
        )

    def hand(u):
        spot, h = lax.rem(u // H, ring), lax.rem(u, H)
        return pltpu.make_async_remote_copy(
            src_ref=vbuf.at[spot, h, :, :, mid],
            dst_ref=vbuf.at[spot, h, :, :, low],
            send_sem=gsnd.at[lax.rem(u, SLOTS)],
            recv_sem=grcv.at[lax.rem(u, SLOTS)],
            device_id={"row": 1 - my_row},
            device_id_type=MESH,
        )

    def begin(u):
        return jnp.where((my_row == 0) & (is_early(u)), 1, 0) if zone else 0

    def swap_factors():
        for j in range(1, groups):
            pass_factors(j).wait_send()
            part = tbuf.at[pl.ds(lax.rem(my_row + groups - j, groups) * share, share)]
            pltpu.make_async_remote_copy(
                src_ref=part,
                dst_ref=part,
                send_sem=tsnd.at[j - 1],
                recv_sem=trcv.at[j - 1],
                device_id={"row": lax.rem(my_row + j, groups)},
                device_id_type=MESH,
            ).wait_recv()

    def partial(sl, j):
        return pltpu.make_async_remote_copy(
            src_ref=psend.at[sl],
            dst_ref=precv.at[sl, j - 1],
            send_sem=psnd.at[sl, j - 1],
            recv_sem=prcv.at[sl, j - 1],
            device_id={"row": lax.rem(my_row + j, groups)},
            device_id_type=MESH,
        )

    def project(u):
        spot, h = lax.rem(u // H, ring), lax.rem(u, H)
        sl = lax.rem(u, 2 * H)
        if zone:

            @pl.when((my_row == 1) & (is_early(u)))
            def _():
                hand(u).wait_recv()

        part = pl.ds(0, members * sub)
        acc[part] = jnp.zeros((members * sub, acc.shape[1]), jnp.float32)

        def body(n, _):
            at = pl.multiple_of(n * tile, tile)
            left = halves(vbuf[spot, h, :, :, pl.ds(at, tile)].reshape(members * sub, tile))
            right = halves(zbuf[pl.ds(at, tile), :])
            acc[part] += dot3(left, right, 1, 0)
            return 0

        lax.fori_loop(begin(u), rows // tile, body, 0)
        psend[sl] = acc[part]
        for j in range(1, groups):
            partial(sl, j).start()

    def store(n):
        spot = pl.ds(pl.multiple_of(n * tile, tile), tile)
        return pltpu.make_async_copy(zbuf.at[spot], out_ref.at[spot], zsem)

    def update(i, last):
        base = lax.rem(i, 2) * H
        total = []
        for h in range(H):
            whole_sum = psend[base + h]
            for j in range(1, groups):
                partial(base + h, j).wait()
                whole_sum = whole_sum + precv[base + h, j - 1]
            total.append(whole_sum)
        total = halves(jnp.concatenate(total, axis=0))
        spot = lax.rem(i, ring)
        factor = halves(tbuf[panels - 1 - i].reshape(width, width))
        scaled = dot3(factor, total, 0, 0)
        for h in range(H):
            for owner in range(members):
                at = (owner * H + h) * sub
                acc[pl.ds((h * members + owner) * sub, sub), :] = scaled[at : at + sub]
        scaled = halves(acc[...])

        def body(n, _):
            at = pl.multiple_of(n * tile, tile)
            left = halves(vbuf[spot, :, :, :, pl.ds(at, tile)].reshape(width, tile))
            zbuf[pl.ds(at, tile), :] = zbuf[pl.ds(at, tile), :] - dot3(left, scaled, 0, 0)
            if last:

                @pl.when(n > 0)
                def _():
                    store(n - 1).start()

            return 0

        lax.fori_loop(0 if last else begin(i * H + H - 1), rows // tile, body, 0)

    barrier = pltpu.get_barrier_semaphore()

    def greet(target):
        pl.semaphore_signal(barrier, inc=1, device_id=target, device_id_type=MESH)

    pl.when(a < A - 1)(lambda: greet({"col": index(a + 1, b, c)}))
    pl.when(a > 0)(lambda: greet({"col": index(a - 1, b, c)}))
    for j in range(1, B):
        greet({"col": index(a, lax.rem(b + j, B), c)})
    greet({"col": index(a, b, 1 - c)})
    for j in range(1, groups):
        greet({"row": lax.rem(my_row + j, groups)})
    beyond = jnp.where(a < A - 1, 1, 0) + jnp.where(a > 0, 1, 0)
    pl.semaphore_wait(barrier, beyond + (B + groups - 1))

    fetch = pltpu.make_async_copy(z_hbm, zbuf, zsem)
    if zone:

        @pl.when(my_row == 1)
        def _():
            lend().start()

    hop(jnp.int32(0), 0, True)
    for u in range(1, AHEAD):
        hop(jnp.int32(u), 0, True, (0,))
    fetch.start()
    own_factors().start()
    if zone:

        @pl.when(my_row == 0)
        def _():
            lend().wait_recv()

    for u in range(1, AHEAD):
        hop(jnp.int32(u), 0, True, (1,))
    fetch.wait()

    def slot(t, _):
        w = t - A

        @pl.when((w >= 0) & (w < units))
        def _():
            i, h = w // H, lax.rem(w, H)

            @pl.when((h == 0) & (i == 1))
            def _():
                swap_factors()

            @pl.when((h == 0) & (w > 0))
            def _():
                update(i - 1, False)

            project(w)

        for h in range(A, 0, -1):
            u = t - (h - 1)

            @pl.when((u >= 0) & (u < units))
            def _(u=u, h=h):
                hop(u, h, True)

        @pl.when(t + AHEAD < units)
        def _():
            hop(t + AHEAD, 0, True)

        v = t - A + 1

        @pl.when((v >= 0) & (v < units))
        def _():
            settle(v)

        for h in range(A + 1):
            u = t - (SENDS - 1) - (h - 1 if h else -AHEAD)

            @pl.when((u >= 0) & (u < units))
            def _(u=u, h=h):
                hop(u, h, False)

        if zone:

            @pl.when((my_row == 0) & is_early(w))
            def _():
                hand(w).wait_send()

        return 0

    lax.fori_loop(0, units + A + SENDS - 2, slot, 0)
    update(jnp.int32(panels - 1), True)
    if zone:

        @pl.when(my_row == 1)
        def _():
            lend().wait_send()

    store(rows // tile - 1).start()
    pltpu.make_async_copy(zbuf, out_ref, zsem).wait()


def local(eigvecs, v_panels, t_panels):
    panels, rows, per = v_panels.shape
    width = t_panels.shape[1]
    groups = lax.axis_size("row")
    members = lax.axis_size("col")
    chips = members // 2
    B = max(n for n in range(1, chips + 1) if chips % n == 0 and n * n <= chips)
    A = chips // B
    columns = eigvecs.shape[1]
    H = per // 8 if per % 8 == 0 else 1
    sub = per // H
    vectors = jnp.transpose(v_panels, (0, 2, 1)).reshape(panels, H, sub, rows)
    factors = jnp.transpose(t_panels, (0, 2, 1)).reshape(panels, H, sub, width)
    dma = pltpu.SemaphoreType.DMA
    anywhere = pl.BlockSpec(memory_space=pl.ANY)
    others = max(groups - 1, 1)
    ring = min(panels, 1 + (A + AHEAD + 2 + H - 1) // H)
    tile = min(rows, 1024)
    zone = tile if groups == 2 and rows >= 4 * tile and tile % (2 * width) == 0 and tile < panels * width else 0
    lent = (panels - zone // width, H, sub, zone // 2) if zone else (1, H, sub, 128)
    out = pl.pallas_call(
        functools.partial(kernel, (groups, A, B, zone, tile)),
        out_shape=jax.ShapeDtypeStruct((rows, columns), jnp.float32),
        in_specs=[anywhere] * 3,
        out_specs=anywhere,
        scratch_shapes=[
            pltpu.VMEM((rows, columns), jnp.float32),
            pltpu.VMEM((ring, H, members, sub, rows), jnp.float32),
            pltpu.VMEM((panels, H, members, sub, width), jnp.float32),
            pltpu.VMEM(lent, jnp.float32),
            pltpu.VMEM((width, columns), jnp.float32),
            pltpu.VMEM((2 * H, members * sub, columns), jnp.float32),
            pltpu.VMEM((2 * H, others, members * sub, columns), jnp.float32),
            dma((SLOTS, chips)),
            dma((SLOTS, A * max(B - 1, 1))),
            dma((SLOTS, chips)),
            dma((SENDS, chips)),
            dma((SENDS, chips)),
            dma((SENDS, A + 1, max(B - 1, 1))),
            dma((SENDS, chips)),
            dma((A,)),
            dma((A,)),
            dma((A, max(B - 1, 1))),
            dma((chips,)),
            dma((2, chips)),
            dma((SLOTS,)),
            dma,
            dma((2 * H, others)),
            dma((2 * H, others)),
            dma,
            dma((others,)),
            dma((others,)),
            dma,
            dma,
            dma((SLOTS,)),
            dma((SLOTS,)),
        ],
        compiler_params=pltpu.CompilerParams(
            collective_id=0, has_side_effects=True, vmem_limit_bytes=54 * 2**20
        ),
    )(eigvecs, vectors, factors)
    return out


def solution(mesh):
    in_specs = (P("row", "col"), P(None, "row", "col"), P(None, None, "col"))
    out_specs = P("row", "col")
    return jax.shard_map(local, mesh=mesh, in_specs=in_specs, out_specs=out_specs, check_vma=False)
```

```python
import functools

import jax
import jax.numpy as jnp
from jax import lax
from jax.experimental import pallas as pl
from jax.experimental.pallas import tpu as pltpu
from jax.sharding import PartitionSpec as P

SLOTS = 8
SENDS = 3
AHEAD = 2
MESH = pl.DeviceIdType.MESH


def halves(x):
    high = x.astype(jnp.bfloat16)
    return high, (x - high.astype(jnp.float32)).astype(jnp.bfloat16)


def dot3(left, right, left_axis, right_axis):
    def one(a, b):
        return lax.dot_general(
            a, b, (((left_axis,), (right_axis,)), ((), ())), preferred_element_type=jnp.float32
        )

    (lh, ll), (rh, rl) = left, right
    return one(jnp.concatenate([lh, ll, lh], left_axis), jnp.concatenate([rh, rh, rl], right_axis))


def kernel(shape, z_hbm, v_ref, t_ref, out_ref, zbuf, vbuf, tbuf, stage, acc, psend, precv, *sems):
    groups, A, B, zone, tile = shape
    recv, rside, rpair, su, sd, sy, sc, tu, td, ty, tc, tr = sems[:12]
    lsem, zsem, psnd, prcv, town, tsnd, trcv, lsnd, lrcv, gsnd, grcv = sems[12:]
    panels, H, sub, rows = v_ref.shape
    members = 2 * A * B
    ring = vbuf.shape[0]
    width = H * members * sub
    units = panels * H
    share = panels // groups
    tiles = rows // 128
    spare = (B - 1) * A - (A - 1)
    whole = 2 * max((A - 1) * (B - 1), 1)
    side = min(max((tiles * spare + whole // 2) // whole, 1), tiles - 1)
    cut = (tiles - side) * 128
    half = zone // 2

    def is_early(u):
        return (u > 0) & (u < early)

    floor = zone // width
    early = (panels - floor) * H if zone else 0
    me = lax.axis_index("col")
    my_row = lax.axis_index("row")
    c = lax.rem(me, 2)
    b = lax.rem(me // 2, B)
    a = me // (2 * B)
    mine = pl.ds(my_row * share, share)

    def index(aa, bb, cc):
        return (aa * B + bb) * 2 + cc

    def place(u, owner, lo, hi):
        return vbuf.at[lax.rem(u // H, ring), lax.rem(u, H), owner, :, pl.ds(lo, hi - lo)]

    def sized(u, body):
        if zone:
            pl.when(is_early(u))(lambda: body(half))
            pl.when(jnp.logical_not(is_early(u)))(lambda: body(0))
        else:
            body(0)

    def landed(spot, sem):
        pltpu.make_async_remote_copy(
            src_ref=spot,
            dst_ref=spot,
            send_sem=sc.at[0, 0],
            recv_sem=sem,
            device_id={"col": index(a, b, 1 - c)},
            device_id_type=MESH,
        ).wait_recv()

    def source(u, span):
        return v_ref.at[panels - 1 - u // H, lax.rem(u, H), :, span]

    def slot_of(u, span):
        return vbuf.at[lax.rem(u // H, ring), lax.rem(u, H), me, :, span]

    def staged(u):
        return stage.at[panels - 1 - u // H - floor, lax.rem(u, H)]

    low, mid, high = pl.ds(0, half), pl.ds(half, zone - half), pl.ds(zone, rows - zone)

    def lent(u, body):
        borrowed = (my_row == 0) & (is_early(u))
        pl.when(borrowed)(lambda: body(staged(u)))

    def hop(u, h, go, stages=(0, 1)):
        sl = lax.rem(u, SLOTS)
        ts = lax.rem(u + (h - 1 if h else SENDS - AHEAD), SENDS)

        def copy(src, dst, target, send_sem, recv_sem):
            return pltpu.make_async_remote_copy(
                src_ref=src,
                dst_ref=dst,
                send_sem=send_sem,
                recv_sem=recv_sem,
                device_id={"col": target},
                device_id_type=MESH,
            )

        def move(owner, stop, target, send_sem, recv_sem):
            def part(src, lo, hi):
                copy(src, place(u, owner, lo, hi), target, send_sem, recv_sem).start()

            def fresh(lo, hi):
                part(source(u, pl.ds(lo, hi - lo)), lo, hi)

            def passed(lo, hi):
                spot = place(u, owner, lo, hi)
                one = copy(spot, spot, target, send_sem, recv_sem)
                one.start() if go else one.wait_send()

            if not go or h:
                if stop is None:
                    passed(cut, rows)
                else:
                    sized(u, lambda start: passed(start, stop))
            elif stop is None:
                if 0 in stages:
                    fresh(cut, rows)
            elif zone:
                borrowed = (my_row == 0) & (is_early(u))
                if 0 in stages:
                    pl.when(borrowed)(lambda: fresh(zone, stop))
                    pl.when(jnp.logical_not(borrowed) & (is_early(u)))(lambda: fresh(half, stop))
                    pl.when(jnp.logical_not(is_early(u)))(lambda: fresh(0, stop))
                if 1 in stages:
                    pl.when(borrowed)(lambda: part(staged(u), half, zone))
            elif 0 in stages:
                fresh(0, stop)

        def move_factor(owner, target, send_sem, recv_sem):
            spot = tbuf.at[mine, :, owner]
            one = copy(spot if h else t_ref.at[mine], spot, target, send_sem, recv_sem)
            one.start() if go else one.wait_send()

        def both(sg, body):
            if sg >= 0:
                pl.when(a < A - 1)(lambda: body(index(a + 1, b, c), 0))
            if sg <= 0:
                pl.when(a > 0)(lambda: body(index(a - 1, b, c), 1))

        def signs(d):
            return (1, -1) if d else (0,)

        def facing(d, body):
            if d < A:
                for sg in signs(d):
                    at = a - sg * d
                    if d == 0:
                        body(sg, at)
                    else:
                        pl.when((at >= 0) & (at < A))(functools.partial(body, sg, at))

        def forward(sg, at):
            owner, cid = index(at, b, c), at * B + b
            both(sg, lambda to, way: move(owner, rows, to, (su, sd)[way].at[ts, at * B], recv.at[sl, cid]))
            for j in range(1, B):
                to = index(a, lax.rem(b + j, B), c)
                if h == 0:
                    side = at * (B - 1) + (B - j - 1)
                    move(owner, None, to, sy.at[ts, A, j - 1], rside.at[sl, side])
                move(owner, cut, to, sy.at[ts, at, j - 1], recv.at[sl, cid])
            move(owner, rows, index(a, b, 1 - c), sc.at[ts, cid], rpair.at[sl, cid])

            if 0 in stages:

                @pl.when(u == 0)
                def _():
                    both(sg, lambda to, way: move_factor(owner, to, (tu, td)[way].at[at], tr.at[0, cid]))
                    for j in range(1, B):
                        to = index(a, lax.rem(b + j, B), c)
                        move_factor(owner, to, ty.at[at, j - 1], tr.at[0, cid])
                    move_factor(owner, index(a, b, 1 - c), tc.at[cid], tr.at[1, cid])

        def straight(sg, at):
            owner, cid = index(at, b, c), at * B + b
            if go:
                sized(u, lambda start: landed(place(u, owner, start, rows), recv.at[sl, cid]))
                pl.when(u == 0)(lambda: landed(tbuf.at[mine, :, owner], tr.at[0, cid]))
            forward(sg, at)

        def turned(sg, at):
            for j in range(1, B):
                owner, side = index(at, lax.rem(b + j, B), c), at * (B - 1) + (j - 1)
                if go:
                    landed(place(u, owner, cut, rows), rside.at[sl, side])
                both(sg, lambda to, way: move(owner, None, to, (su, sd)[way].at[ts, at * B + j], rside.at[sl, side]))

        def crossed(sg, at):
            for j in range(1, B):
                bb = lax.rem(b + j, B)
                owner, cid = index(at, bb, c), at * B + bb
                if go:
                    sized(u, lambda start: landed(place(u, owner, start, cut), recv.at[sl, cid]))
                    pl.when(u == 0)(lambda: landed(tbuf.at[mine, :, owner], tr.at[0, cid]))
                move(owner, rows, index(a, b, 1 - c), sc.at[ts, cid], rpair.at[sl, cid])

                @pl.when(u == 0)
                def _():
                    move_factor(owner, index(a, b, 1 - c), tc.at[cid], tr.at[1, cid])

        if h == 0:
            forward(0, a)
            if 1 in stages and go:
                own_vectors(u)
            return

        facing(h, straight)
        facing(h - 1, turned)
        facing(h - 1, crossed)

    def pass_factors(j):
        return pltpu.make_async_remote_copy(
            src_ref=tbuf.at[mine],
            dst_ref=tbuf.at[mine],
            send_sem=tsnd.at[j - 1],
            recv_sem=trcv.at[j - 1],
            device_id={"row": lax.rem(my_row + j, groups)},
            device_id_type=MESH,
        )

    def own_factors():
        return pltpu.make_async_copy(t_ref.at[mine], tbuf.at[mine, :, me], town)

    def settle(u):
        for at in range(A):
            for bb in range(B):
                owner, sem = index(at, bb, 1 - c), rpair.at[lax.rem(u, SLOTS), at * B + bb]
                sized(u, lambda start: landed(place(u, owner, start, rows), sem))

        if zone:

            @pl.when(jnp.logical_not(is_early(u)))
            def _():
                own_arrived(u, pl.ds(0, rows))

            @pl.when(is_early(u))
            def _():
                own_arrived(u, pl.ds(half, rows - half))

                @pl.when(my_row == 0)
                def _():
                    hand(u).start()
        else:
            own_arrived(u, pl.ds(0, rows))

        @pl.when(u == 0)
        def _():
            for at in range(A):
                for bb in range(B):
                    landed(tbuf.at[mine, :, index(at, bb, 1 - c)], tr.at[1, at * B + bb])
            own_factors().wait()
            for j in range(1, groups):
                pass_factors(j).start()

    def own_vectors(u):
        def fetch_own(src, span):
            pltpu.make_async_copy(src, slot_of(u, span), lsem.at[lax.rem(u, SLOTS)]).start()

        if zone:
            lent(u, lambda src: fetch_own(src, mid))
            rest = pl.ds(half, rows - half)
            borrowed = (my_row == 0) & (is_early(u))
            pl.when(borrowed)(lambda: fetch_own(source(u, high), high))
            pl.when(jnp.logical_not(borrowed) & (is_early(u)))(lambda: fetch_own(source(u, rest), rest))
            pl.when(jnp.logical_not(is_early(u)))(lambda: fetch_own(source(u, pl.ds(0, rows)), pl.ds(0, rows)))
        else:
            fetch_own(source(u, pl.ds(0, rows)), pl.ds(0, rows))

    def own_arrived(u, span):
        pltpu.make_async_copy(source(u, span), slot_of(u, span), lsem.at[lax.rem(u, SLOTS)]).wait()

    def lend():
        return pltpu.make_async_remote_copy(
            src_ref=v_ref.at[pl.ds(floor, panels - floor), :, :, low],
            dst_ref=stage,
            send_sem=lsnd,
            recv_sem=lrcv,
            device_id={"row": 1 - my_row},
            device_id_type=MESH,
        )

    def hand(u):
        spot, h = lax.rem(u // H, ring), lax.rem(u, H)
        return pltpu.make_async_remote_copy(
            src_ref=vbuf.at[spot, h, :, :, mid],
            dst_ref=vbuf.at[spot, h, :, :, low],
            send_sem=gsnd.at[lax.rem(u, SLOTS)],
            recv_sem=grcv.at[lax.rem(u, SLOTS)],
            device_id={"row": 1 - my_row},
            device_id_type=MESH,
        )

    def begin(u):
        return jnp.where((my_row == 0) & (is_early(u)), 1, 0) if zone else 0

    def swap_factors():
        for j in range(1, groups):
            pass_factors(j).wait_send()
            part = tbuf.at[pl.ds(lax.rem(my_row + groups - j, groups) * share, share)]
            pltpu.make_async_remote_copy(
                src_ref=part,
                dst_ref=part,
                send_sem=tsnd.at[j - 1],
                recv_sem=trcv.at[j - 1],
                device_id={"row": lax.rem(my_row + j, groups)},
                device_id_type=MESH,
            ).wait_recv()

    def partial(sl, j):
        return pltpu.make_async_remote_copy(
            src_ref=psend.at[sl],
            dst_ref=precv.at[sl, j - 1],
            send_sem=psnd.at[sl, j - 1],
            recv_sem=prcv.at[sl, j - 1],
            device_id={"row": lax.rem(my_row + j, groups)},
            device_id_type=MESH,
        )

    def project(u):
        spot, h = lax.rem(u // H, ring), lax.rem(u, H)
        sl = lax.rem(u, 2 * H)
        if zone:

            @pl.when((my_row == 1) & (is_early(u)))
            def _():
                hand(u).wait_recv()

        part = pl.ds(0, members * sub)
        acc[part] = jnp.zeros((members * sub, acc.shape[1]), jnp.float32)

        def body(n, _):
            at = pl.multiple_of(n * tile, tile)
            left = halves(vbuf[spot, h, :, :, pl.ds(at, tile)].reshape(members * sub, tile))
            right = halves(zbuf[pl.ds(at, tile), :])
            acc[part] += dot3(left, right, 1, 0)
            return 0

        lax.fori_loop(begin(u), rows // tile, body, 0)
        psend[sl] = acc[part]
        for j in range(1, groups):
            partial(sl, j).start()

    def store(n):
        spot = pl.ds(pl.multiple_of(n * tile, tile), tile)
        return pltpu.make_async_copy(zbuf.at[spot], out_ref.at[spot], zsem)

    def update(i, last):
        base = lax.rem(i, 2) * H
        total = []
        for h in range(H):
            whole_sum = psend[base + h]
            for j in range(1, groups):
                partial(base + h, j).wait()
                whole_sum = whole_sum + precv[base + h, j - 1]
            total.append(whole_sum)
        total = halves(jnp.concatenate(total, axis=0))
        spot = lax.rem(i, ring)
        factor = halves(tbuf[panels - 1 - i].reshape(width, width))
        scaled = dot3(factor, total, 0, 0)
        for h in range(H):
            for owner in range(members):
                at = (owner * H + h) * sub
                acc[pl.ds((h * members + owner) * sub, sub), :] = scaled[at : at + sub]
        scaled = halves(acc[...])

        def body(n, _):
            at = pl.multiple_of(n * tile, tile)
            left = halves(vbuf[spot, :, :, :, pl.ds(at, tile)].reshape(width, tile))
            zbuf[pl.ds(at, tile), :] = zbuf[pl.ds(at, tile), :] - dot3(left, scaled, 0, 0)
            if last:

                @pl.when(n > 0)
                def _():
                    store(n - 1).start()

            return 0

        lax.fori_loop(0 if last else begin(i * H + H - 1), rows // tile, body, 0)

    barrier = pltpu.get_barrier_semaphore()

    def greet(target):
        pl.semaphore_signal(barrier, inc=1, device_id=target, device_id_type=MESH)

    pl.when(a < A - 1)(lambda: greet({"col": index(a + 1, b, c)}))
    pl.when(a > 0)(lambda: greet({"col": index(a - 1, b, c)}))
    for j in range(1, B):
        greet({"col": index(a, lax.rem(b + j, B), c)})
    greet({"col": index(a, b, 1 - c)})
    for j in range(1, groups):
        greet({"row": lax.rem(my_row + j, groups)})
    beyond = jnp.where(a < A - 1, 1, 0) + jnp.where(a > 0, 1, 0)
    pl.semaphore_wait(barrier, beyond + (B + groups - 1))

    fetch = pltpu.make_async_copy(z_hbm, zbuf, zsem)
    if zone:

        @pl.when(my_row == 1)
        def _():
            lend().start()

    hop(jnp.int32(0), 0, True)
    for u in range(1, AHEAD):
        hop(jnp.int32(u), 0, True, (0,))
    fetch.start()
    own_factors().start()
    if zone:

        @pl.when(my_row == 0)
        def _():
            lend().wait_recv()

    for u in range(1, AHEAD):
        hop(jnp.int32(u), 0, True, (1,))
    fetch.wait()

    def slot(t, _):
        w = t - A

        @pl.when((w >= 0) & (w < units))
        def _():
            i, h = w // H, lax.rem(w, H)

            @pl.when((h == 0) & (i == 1))
            def _():
                swap_factors()

            @pl.when((h == 0) & (w > 0))
            def _():
                update(i - 1, False)

            project(w)

        for h in range(A, 0, -1):
            u = t - (h - 1)

            @pl.when((u >= 0) & (u < units))
            def _(u=u, h=h):
                hop(u, h, True)

        @pl.when(t + AHEAD < units)
        def _():
            hop(t + AHEAD, 0, True)

        v = t - A + 1

        @pl.when((v >= 0) & (v < units))
        def _():
            settle(v)

        for h in range(A + 1):
            u = t - (SENDS - 1) - (h - 1 if h else -AHEAD)

            @pl.when((u >= 0) & (u < units))
            def _(u=u, h=h):
                hop(u, h, False)

        if zone:

            @pl.when((my_row == 0) & is_early(w))
            def _():
                hand(w).wait_send()

        return 0

    lax.fori_loop(0, units + A + SENDS - 2, slot, 0)
    update(jnp.int32(panels - 1), True)
    if zone:

        @pl.when(my_row == 1)
        def _():
            lend().wait_send()

    store(rows // tile - 1).start()
    pltpu.make_async_copy(zbuf, out_ref, zsem).wait()


def local(eigvecs, v_panels, t_panels):
    panels, rows, per = v_panels.shape
    width = t_panels.shape[1]
    groups = lax.axis_size("row")
    members = lax.axis_size("col")
    chips = members // 2
    B = max(n for n in range(1, chips + 1) if chips % n == 0 and n * n <= chips)
    A = chips // B
    columns = eigvecs.shape[1]
    H = per // 8 if per % 8 == 0 else 1
    sub = per // H
    vectors = jnp.transpose(v_panels, (0, 2, 1)).reshape(panels, H, sub, rows)
    factors = jnp.transpose(t_panels, (0, 2, 1)).reshape(panels, H, sub, width)
    dma = pltpu.SemaphoreType.DMA
    anywhere = pl.BlockSpec(memory_space=pl.ANY)
    others = max(groups - 1, 1)
    ring = min(panels, 1 + (A + AHEAD + 2 + H - 1) // H)
    tile = min(rows, 1024)
    zone = tile if groups == 2 and rows >= 4 * tile and tile % (2 * width) == 0 and tile < panels * width else 0
    lent = (panels - zone // width, H, sub, zone // 2) if zone else (1, H, sub, 128)
    out = pl.pallas_call(
        functools.partial(kernel, (groups, A, B, zone, tile)),
        out_shape=jax.ShapeDtypeStruct((rows, columns), jnp.float32),
        in_specs=[anywhere] * 3,
        out_specs=anywhere,
        scratch_shapes=[
            pltpu.VMEM((rows, columns), jnp.float32),
            pltpu.VMEM((ring, H, members, sub, rows), jnp.float32),
            pltpu.VMEM((panels, H, members, sub, width), jnp.float32),
            pltpu.VMEM(lent, jnp.float32),
            pltpu.VMEM((width, columns), jnp.float32),
            pltpu.VMEM((2 * H, members * sub, columns), jnp.float32),
            pltpu.VMEM((2 * H, others, members * sub, columns), jnp.float32),
            dma((SLOTS, chips)),
            dma((SLOTS, A * max(B - 1, 1))),
            dma((SLOTS, chips)),
            dma((SENDS, chips)),
            dma((SENDS, chips)),
            dma((SENDS, A + 1, max(B - 1, 1))),
            dma((SENDS, chips)),
            dma((A,)),
            dma((A,)),
            dma((A, max(B - 1, 1))),
            dma((chips,)),
            dma((2, chips)),
            dma((SLOTS,)),
            dma,
            dma((2 * H, others)),
            dma((2 * H, others)),
            dma,
            dma((others,)),
            dma((others,)),
            dma,
            dma,
            dma((SLOTS,)),
            dma((SLOTS,)),
        ],
        compiler_params=pltpu.CompilerParams(
            collective_id=0, has_side_effects=True, vmem_limit_bytes=54 * 2**20
        ),
    )(eigvecs, vectors, factors)
    return out


def solution(mesh):
    in_specs = (P("row", "col"), P(None, "row", "col"), P(None, None, "col"))
    out_specs = P("row", "col")
    return jax.shard_map(local, mesh=mesh, in_specs=in_specs, out_specs=out_specs, check_vma=False)
```
